32 devices in a mesh: cat: 2 (over x), lat: 4 (over y, core), lon: 4 (over z).
Axes of the slice: x: 2, y: 2, z: 4, core: 2. Of those that a mesh axis runs over, the one named last changes fastest.
Arguments:
- thickness: bfloat16 [40, 1024, 2560], P('cat', 'lat', 'lon'), may hold values from 0.099609375 to 4
- area: bfloat16 [40, 1024, 2560], P('cat', 'lat', 'lon'), may hold values from 0.0049743652 to 0.049804688
- ridge_weight: float32 [40], P('cat'), may hold values from 0.2 to 2
- cat_top: int32 [1024, 2560], P('lat', 'lon'), may hold values from 1 to 40
- land_mask: int32 [1024, 2560], P('lat', 'lon'), may hold values 0 or 1
- velocity_u: float32 [1024, 2560], P('lat', 'lon'), may hold values from -1.8 to 1.8
- velocity_v: float32 [1024, 2560], P('lat', 'lon'), may hold values from -1.8 to 1.8
- stress_div: float32 [1024, 2560], P('lat', 'lon'), may hold values from -3 to 3
- stress_ten: float32 [1024, 2560], P('lat', 'lon'), may hold values from -3 to 3
- stress_shear: float32 [1024, 2560], P('lat', 'lon'), may hold values from -3 to 3
- wind_x: float32 [1024, 2560], P('lat', 'lon'), may hold values from -6 to 6
- wind_y: float32 [1024, 2560], P('lat', 'lon'), may hold values from -6 to 6
- water_drag: float32 [1024, 2560], P('lat', 'lon'), may hold values from 0.2 to 2
Outputs:
- new_u: float32 [1024, 2560], P('lat', 'lon')
- new_v: float32 [1024, 2560], P('lat', 'lon')
- new_div: float32 [1024, 2560], P('lat', 'lon')
- new_ten: float32 [1024, 2560], P('lat', 'lon')
- new_shear: float32 [1024, 2560], P('lat', 'lon')
The draws below stay inside these ranges and needn't reach their ends.
Inputs may be any that keep to these rules, and one draw needn't show every extreme that they name: Categories with index cat_top or above are absent from a cell.
All inputs are finite; a program needn't handle non-finite values. No bound on the sum of `land_mask` on one device may be relied on, other than what follows from the above.
Results may differ from the reference program's by a relative error of at most 0.0003.
Values sent between devices are 32-bit elements; how exact they have to be, the bound alone decides.
A program may use at most 128 MiB of HBM per device.

```python
import math
import jax
import jax.numpy as jnp
from jax import lax

NCAT = 40
SUB = 4
NLAT = 1024
NLON = 2560


def with_ends(entries, stream_key, least, high):
    shape = entries.shape
    spot = [jax.random.randint(jax.random.fold_in(stream_key, axis), (), 0, shape[axis]) for axis in range(len(shape))]
    entries = entries.at[tuple(spot)].set(least)
    longest = shape.index(max(shape))
    spot[longest] = (spot[longest] + 1) % shape[longest]
    return entries.at[tuple(spot)].set(high)


def shard_levels(rng, extent, cuts, low, high):
    factor_of = 1.0
    for axis_at, shards_of in cuts:
        steps = jax.random.uniform(jax.random.fold_in(jax.random.fold_in(rng, 6), axis_at), (shards_of,), jnp.float32, low / len(cuts), high / len(cuts))
        factor_of = factor_of * jnp.repeat(jnp.exp(steps), extent[axis_at] // shards_of).reshape((-1,) + (1,) * (len(extent) - 1 - axis_at))
    return factor_of


def noise(own_key, shape, deviation, limit, cuts=(), dtype=jnp.bfloat16):
    drawn = jax.random.normal(own_key, shape, jnp.float32) * deviation
    if len(cuts) > 0:
        drawn = shard_levels(own_key, shape, cuts, -0.22, 0.18) * drawn
    return jnp.clip(drawn, min=-limit, max=limit).astype(dtype)


def setup_inputs(seed: int = 0) -> dict:
    streams_of = jax.random.split(jax.random.key(seed), 14)
    return {
        "thickness": jnp.clip(jnp.exp(math.log(4.0) - 3.6927934 * jax.random.uniform(streams_of[0], (NCAT, NLAT, NLON), jnp.float32) ** shard_levels(streams_of[0], (NCAT, NLAT, NLON), ((0, 2), (1, 4), (2, 4)), -0.2, 0.2)), 0.099609375, 4.0).astype(jnp.bfloat16),
        "area": jnp.clip(jnp.exp(math.log(0.049804688) - 2.3038113 * jax.random.uniform(streams_of[1], (NCAT, NLAT, NLON), jnp.float32) ** shard_levels(streams_of[1], (NCAT, NLAT, NLON), ((0, 2), (1, 4), (2, 4)), -0.2, 0.2)), 0.0049743652, 0.049804688).astype(jnp.bfloat16),
        "ridge_weight": jnp.clip(jnp.exp(math.log(2.0) - 2.3025851 * jax.random.uniform(streams_of[2], (NCAT,), jnp.float32) ** shard_levels(streams_of[2], (NCAT,), ((0, 2),), -0.2, 0.2)), 0.2, 2.0),
        "cat_top": with_ends(jax.random.randint(streams_of[3], (NLAT, NLON), 1, NCAT + 1), jax.random.fold_in(streams_of[3], 1), 1, NCAT).astype(jnp.int32),
        "land_mask": with_ends((jax.random.randint(streams_of[4], (NLAT, NLON), 0, 10) < 9).astype(jnp.int32), jax.random.fold_in(streams_of[4], 1), 0, 1),
        "velocity_u": noise(streams_of[5], (NLAT, NLON), 0.3, 1.8, ((0, 4), (1, 4)), jnp.float32),
        "velocity_v": noise(streams_of[6], (NLAT, NLON), 0.3, 1.8, ((0, 4), (1, 4)), jnp.float32),
        "stress_div": noise(streams_of[7], (NLAT, NLON), 0.5, 3.0, ((0, 4), (1, 4)), jnp.float32),
        "stress_ten": noise(streams_of[8], (NLAT, NLON), 0.5, 3.0, ((0, 4), (1, 4)), jnp.float32),
        "stress_shear": noise(streams_of[9], (NLAT, NLON), 0.5, 3.0, ((0, 4), (1, 4)), jnp.float32),
        "wind_x": noise(streams_of[10], (NLAT, NLON), 1.0, 6.0, ((0, 4), (1, 4)), jnp.float32),
        "wind_y": noise(streams_of[11], (NLAT, NLON), 1.0, 6.0, ((0, 4), (1, 4)), jnp.float32),
        "water_drag": jnp.clip(jnp.exp(math.log(2.0) - 2.3025851 * jax.random.uniform(streams_of[12], (NLAT, NLON), jnp.float32) ** shard_levels(streams_of[12], (NLAT, NLON), ((0, 4), (1, 4)), -0.2, 0.2)), 0.2, 2.0),
    }


ELASTIC = 2.0
ECC_SQUARED = 4.0
DELTA_FLOOR = 0.05
CORIOLIS = 0.5

def slopes(along, across):
    return (0.5 * (along[:, :, 2:] - along[:, :, :-2]), 0.5 * (across[:, 2:, :] - across[:, :-2, :]))

def global_pad(along_stack, across_stack):
    along = jnp.pad(along_stack, ((0, 0), (0, 0), (1, 1)), mode='wrap')
    across = jnp.pad(across_stack, ((0, 0), (1, 1), (0, 0)))
    return (along, across)

def subcycle(velocity, stresses, statics):
    strength, mass, concentration, drag, push_x, push_y, wet = statics
    along, across = global_pad(velocity, velocity)
    ddx, ddy = slopes(along, across)
    divergence = ddx[0] + ddy[1]
    tension = ddx[0] - ddy[1]
    shearing = ddy[0] + ddx[1]
    delta = jnp.sqrt(divergence * divergence + (tension * tension + shearing * shearing) / ECC_SQUARED + DELTA_FLOOR * DELTA_FLOOR)
    relax = 1.0 / (1.0 + ELASTIC)
    viscous = ELASTIC * strength / delta
    first = wet * (stresses[0] + viscous * (divergence - delta)) * relax
    second = wet * (stresses[1] + viscous * tension / ECC_SQUARED) * relax
    cross = wet * (stresses[2] + viscous * shearing / ECC_SQUARED) * relax
    normal_x = 0.5 * (first + second)
    normal_y = 0.5 * (first - second)
    along_s, across_s = global_pad(jnp.stack([normal_x, cross]), jnp.stack([cross, normal_y]))
    sdx, sdy = slopes(along_s, across_s)
    force_x = sdx[0] + sdy[0]
    force_y = sdx[1] + sdy[1]
    denom = mass + drag + 1.0 - wet
    speed_u = wet * (mass * velocity[0] + force_x + concentration * push_x + CORIOLIS * mass * velocity[1]) / denom
    speed_v = wet * (mass * velocity[1] + force_y + concentration * push_y - CORIOLIS * mass * velocity[0]) / denom
    return (jnp.stack([speed_u, speed_v]), jnp.stack([first, second, cross]))

def reference(thickness, area, ridge_weight, cat_top, land_mask, velocity_u, velocity_v, stress_div, stress_ten, stress_shear, wind_x, wind_y, water_drag):

    def accumulate(level, carry):
        strength, mass, concentration = carry
        height = lax.dynamic_index_in_dim(thickness, level, 0, keepdims=False).astype(jnp.float32)
        present = (level < cat_top).astype(jnp.float32)
        cover = lax.dynamic_index_in_dim(area, level, 0, keepdims=False).astype(jnp.float32) * present
        weight = lax.dynamic_index_in_dim(ridge_weight, level, 0, keepdims=False)
        return (strength + weight * cover * height * height, mass + cover * height, concentration + cover)
    zeros = jnp.zeros(cat_top.shape, jnp.float32)
    strength, mass, concentration = lax.fori_loop(jnp.int32(0), jnp.int32(NCAT), accumulate, (zeros, zeros, zeros))
    wet = land_mask.astype(jnp.float32)
    statics = (strength, mass, concentration, water_drag, wind_x, wind_y, wet)
    velocity = jnp.stack([velocity_u, velocity_v])
    stresses = jnp.stack([stress_div, stress_ten, stress_shear])
    for step in range(SUB):
        velocity, stresses = subcycle(velocity, stresses, statics)
    return (velocity[0], velocity[1], stresses[0], stresses[1], stresses[2])
```

```python
import functools

import jax
import jax.numpy as jnp
from jax import lax
from jax.experimental import pallas as pl
from jax.experimental.pallas import tpu as pltpu
from jax.sharding import PartitionSpec as P

SUB = 4
LANES = 128
EDGE = 8
BLOCK = 16
CHUNK = 32
FINAL = 16
TOP = 16
FOLD = 4
MESH = pl.DeviceIdType.MESH

FS, FM, FC, FD, FX, FY, FW, FU, FV, FA, FB, FT = range(12)
FIELDS = 12
THIRD = 1.0 / 3.0


def read(field, f, c, r, shift=0):
    if shift == 0:
        return field[f, c, pl.ds(pl.multiple_of(r, EDGE), EDGE), :]
    near = field.at[f, c, pl.ds(pl.multiple_of(r - EDGE, EDGE), 3 * EDGE)]
    return near[EDGE + shift : 2 * EDGE + shift, :]


def put(ref, value, mask):
    if mask is None:
        ref[...] = value
    else:
        pltpu.store(ref, value, mask=mask)


def along(x, lane):
    tiles = len(x)
    ahead = [pltpu.roll(a, LANES - 1, 1) for a in x]
    behind = [pltpu.roll(a, 1, 1) for a in x]
    return [
        jnp.where(lane == LANES - 1, ahead[(c + 1) % tiles], ahead[c])
        - jnp.where(lane == 0, behind[c - 1], behind[c])
        for c in range(tiles)
    ]


def derive(field, r):
    tiles = field.shape[1]
    at = pl.ds(pl.multiple_of(r, EDGE), EDGE)
    for c in range(tiles):
        wet = field[FW, c, at, :]
        mass = field[FM, c, at, :]
        ratio = wet / (mass + field[FD, c, at, :] + 1.0 - wet)
        force = field[FC, c, at, :] * ratio
        field[FS, c, at, :] = (2.0 * THIRD) * wet * field[FS, c, at, :]
        field[FM, c, at, :] = mass * ratio
        field[FD, c, at, :] = 0.25 * ratio
        field[FX, c, at, :] = force * field[FX, c, at, :]
        field[FY, c, at, :] = force * field[FY, c, at, :]
        field[FW, c, at, :] = THIRD * wet
        first = field[FA, c, at, :]
        second = field[FB, c, at, :]
        field[FA, c, at, :] = first + second
        field[FB, c, at, :] = first - second
        field[FT, c, at, :] = 2.0 * field[FT, c, at, :]


def stress(field, outs, r, mask, lane):
    tiles = field.shape[1]
    at = pl.ds(pl.multiple_of(r, EDGE), EDGE)
    dxu = along([field[FU, c, at, :] for c in range(tiles)], lane)
    dxv = along([field[FV, c, at, :] for c in range(tiles)], lane)
    for c in range(tiles):
        dyu = read(field, FU, c, r, 1) - read(field, FU, c, r, -1)
        dyv = read(field, FV, c, r, 1) - read(field, FV, c, r, -1)
        div = dxu[c] + dyv
        ten = dxu[c] - dyv
        shr = dyu + dxv[c]
        inverse = lax.rsqrt(div * div + 0.25 * (ten * ten + shr * shr) + 0.01)
        power = field[FS, c, at, :]
        keep = field[FW, c, at, :]
        gain = power * inverse
        p = gain * div - power
        q = (0.25 * gain) * ten
        a = keep * field[FA, c, at, :] + (p + q)
        b = keep * field[FB, c, at, :] + (p - q)
        s = keep * field[FT, c, at, :] + (0.5 * gain) * shr
        put(field.at[FA, c, at], a, mask)
        put(field.at[FB, c, at], b, mask)
        put(field.at[FT, c, at], s, mask)
        if outs is not None and c < tiles - 1:
            spot = (pl.ds(pl.multiple_of(r - TOP, EDGE), EDGE), pl.ds(c * LANES, LANES))
            put(outs[2].at[spot], 0.5 * (a + b), mask)
            put(outs[3].at[spot], 0.5 * (a - b), mask)
            put(outs[4].at[spot], 0.5 * s, mask)


def motion(field, outs, r, mask, lane):
    tiles = field.shape[1]
    at = pl.ds(pl.multiple_of(r, EDGE), EDGE)
    dxa = along([field[FA, c, at, :] for c in range(tiles)], lane)
    dxt = along([field[FT, c, at, :] for c in range(tiles)], lane)
    for c in range(tiles):
        fx = dxa[c] + (read(field, FT, c, r, 1) - read(field, FT, c, r, -1))
        fy = dxt[c] + (read(field, FB, c, r, 1) - read(field, FB, c, r, -1))
        u = field[FU, c, at, :]
        v = field[FV, c, at, :]
        inertia = field[FM, c, at, :]
        ratio = field[FD, c, at, :]
        new_u = inertia * (u + 0.5 * v) + ratio * fx + field[FX, c, at, :]
        new_v = inertia * (v - 0.5 * u) + ratio * fy + field[FY, c, at, :]
        put(field.at[FU, c, at], new_u, mask)
        put(field.at[FV, c, at], new_v, mask)
        if outs is not None and c < tiles - 1:
            spot = (pl.ds(pl.multiple_of(r - TOP, EDGE), EDGE), pl.ds(c * LANES, LANES))
            put(outs[0].at[spot], new_u, mask)
            put(outs[1].at[spot], new_v, mask)


def sweep(field, outs, start, count, head, tail, skip=()):
    lane = lax.broadcasted_iota(jnp.int32, (EDGE, LANES), 1)
    line = lax.broadcasted_iota(jnp.int32, (EDGE, LANES), 0)

    def half(step, h, emit):
        for k in range(count):
            mask = None
            if k == 0 and head is not None:
                mask = line >= head(h)
            if k == count - 1 and tail is not None:
                mask = line < tail(h)
            step(field, outs if emit and k not in skip else None, start + EDGE * k, mask, lane)

    def cycle(t, carry):
        half(stress, 2 * t, False)
        half(motion, 2 * t + 1, False)
        return carry

    lax.fori_loop(0, SUB - 1, cycle, 0)
    half(stress, 2 * SUB - 2, True)
    half(motion, 2 * SUB - 1, True)


def kernel(
    lat_count,
    lon_count,
    weight,
    thick_hbm,
    area_hbm,
    top_hbm,
    land_hbm,
    u_hbm,
    v_hbm,
    s1_hbm,
    s2_hbm,
    s3_hbm,
    wx_hbm,
    wy_hbm,
    drag_hbm,
    field,
    out_u,
    out_v,
    out_1,
    out_2,
    out_3,
    own,
    other,
    thick,
    area,
    top,
    land,
    pack_left,
    pack_right,
    from_left,
    from_right,
    sum_left,
    sum_right,
    sum_from_left,
    sum_from_right,
    load_sem,
    field_sem,
    x_send,
    x_recv,
    halo_send,
    halo_recv,
):
    outs = (out_u, out_v, out_1, out_2, out_3)
    cats, rows, cols = thick.shape
    tiles = cols // LANES
    halo = tiles
    inner = tiles - 2
    last = cols - LANES
    pieces = rows // CHUNK
    events = (rows - 2 * EDGE - FINAL) // CHUNK
    my_cat = lax.axis_index("cat")
    my_lat = lax.axis_index("lat")
    my_lon = lax.axis_index("lon")
    partner = {"cat": 1 - my_cat}
    west = {"lon": lax.rem(my_lon + lon_count - 1, lon_count)}
    east = {"lon": lax.rem(my_lon + 1, lon_count)}
    north = {"lat": my_lat - 1}
    south = {"lat": my_lat + 1}
    has_north = my_lat > 0
    has_south = my_lat < lat_count - 1

    barrier = pltpu.get_barrier_semaphore()
    for device in (partner, west, east):
        pl.semaphore_signal(barrier, inc=1, device_id=device, device_id_type=MESH)

    @pl.when(has_north)
    def _():
        pl.semaphore_signal(barrier, inc=1, device_id=north, device_id_type=MESH)

    @pl.when(has_south)
    def _():
        pl.semaphore_signal(barrier, inc=1, device_id=south, device_id_type=MESH)

    groups = (
        (0, CHUNK, 0, LANES),
        (CHUNK, rows - CHUNK, 0, LANES),
        (0, rows, last, LANES),
        (0, rows, LANES, cols - 2 * LANES),
    )
    loads = []
    for k, (r0, height, c0, w) in enumerate(groups):
        spot = (pl.ds(r0, height), pl.ds(c0, w))
        group = (
            pltpu.make_async_copy(top_hbm.at[spot], top.at[spot], load_sem.at[3 * k]),
            pltpu.make_async_copy(
                thick_hbm.at[(slice(None),) + spot], thick.at[(slice(None),) + spot], load_sem.at[3 * k + 1]
            ),
            pltpu.make_async_copy(
                area_hbm.at[(slice(None),) + spot], area.at[(slice(None),) + spot], load_sem.at[3 * k + 2]
            ),
        )
        for copy in group:
            copy.start()
        loads.append(group)

    base = my_cat * cats

    def partial(r0, count, c0, w):
        def body(i, carry):
            r = pl.multiple_of(r0 + i * BLOCK, BLOCK)
            at = pl.ds(r, BLOCK)
            for c in range(c0, c0 + w):
                lanes = pl.ds(c * LANES, LANES)
                limit = top[at, lanes] - base
                strength = mass = conc = jnp.zeros((BLOCK, LANES), jnp.float32)
                for n in range(cats):
                    height = thick[n, at, lanes].astype(jnp.float32)
                    cover = jnp.where(limit > n, area[n, at, lanes].astype(jnp.float32), 0.0)
                    volume = cover * height
                    conc = conc + cover
                    mass = mass + volume
                    strength = strength + weight[n] * (volume * height)
                own[0, c, at, :] = strength
                own[1, c, at, :] = mass
                own[2, c, at, :] = conc
            return carry

        lax.fori_loop(0, count, body, 0)

    def exchange(slot, r0, height, c0, w):
        part = (pl.ds(0, 3), pl.ds(c0, w), pl.ds(r0, height))
        return pltpu.make_async_remote_copy(
            src_ref=own.at[part],
            dst_ref=other.at[part],
            send_sem=x_send.at[slot],
            recv_sem=x_recv.at[slot],
            device_id=partner,
            device_id_type=MESH,
        )

    def strip(i, c):
        return exchange((pieces if c else 0) + i, pl.multiple_of(i * CHUNK, CHUNK), CHUNK, c, 1)

    ends = (
        exchange(2 * pieces, 0, EDGE, 1, inner),
        exchange(2 * pieces + 1, rows - EDGE, EDGE, 1, inner),
    )
    final = exchange(2 * pieces + 2, rows - EDGE - FINAL, FINAL, 1, inner)

    def middle(e):
        return exchange(2 * pieces + 3 + e, pl.multiple_of(EDGE + e * CHUNK, EDGE), CHUNK, 1, inner)

    def total(r0, count, c0, w):
        for k in range(count):
            r = pl.multiple_of(r0 + k * EDGE, EDGE)
            at = pl.ds(r, EDGE)
            target = pl.ds(pl.multiple_of(r + TOP, EDGE), EDGE)
            for f in range(3):
                for c in range(c0, c0 + w):
                    field[f, c, target, :] = own[f, c, at, :] + other[f, c, at, :]

    for copy in loads[0]:
        copy.wait()
    partial(0, CHUNK // BLOCK, 0, 1)
    pl.semaphore_wait(barrier, 3 + has_north.astype(jnp.int32) + has_south.astype(jnp.int32))
    strip(0, 0).start()

    def send_strip(c):
        def body(i, carry):
            partial(i * CHUNK, CHUNK // BLOCK, c, 1)
            strip(i, c).start()
            return carry

        return body

    for copy in loads[1]:
        copy.wait()
    lax.fori_loop(1, pieces, send_strip(0), 0)

    land_load = pltpu.make_async_copy(land_hbm, land, load_sem.at[12])
    land_load.start()
    field_loads = []
    for k, (f, ref) in enumerate(
        (
            (FU, u_hbm),
            (FV, v_hbm),
            (FA, s1_hbm),
            (FB, s2_hbm),
            (FT, s3_hbm),
            (FX, wx_hbm),
            (FY, wy_hbm),
            (FD, drag_hbm),
        )
    ):
        for c in range(tiles):
            copy = pltpu.make_async_copy(
                ref.at[:, pl.ds(c * LANES, LANES)],
                field.at[f, c, pl.ds(TOP, rows)],
                field_sem.at[k * tiles + c],
            )
            copy.start()
            field_loads.append(copy)

    @pl.when(jnp.logical_not(has_north))
    def _():
        field[:, :, pl.ds(TOP - EDGE, EDGE), :] = jnp.zeros((FIELDS, tiles + 1, EDGE, LANES), jnp.float32)

    @pl.when(jnp.logical_not(has_south))
    def _():
        field[:, :, pl.ds(TOP + rows, EDGE), :] = jnp.zeros((FIELDS, tiles + 1, EDGE, LANES), jnp.float32)

    for copy in loads[2]:
        copy.wait()
    lax.fori_loop(0, pieces, send_strip(tiles - 1), 0)
    for copy in loads[3]:
        copy.wait()
    partial(0, 1, 1, inner)
    ends[0].start()
    partial(rows - BLOCK, 1, 1, inner)
    ends[1].start()

    def send_middle(e, carry):
        partial(BLOCK + e * CHUNK, CHUNK // BLOCK, 1, inner)
        middle(e).start()
        return carry

    lax.fori_loop(0, events, send_middle, 0)
    final.start()

    land_load.wait()

    def wet_body(i, carry):
        r = pl.multiple_of(i * BLOCK, BLOCK)
        for c in range(tiles):
            field[FW, c, pl.ds(pl.multiple_of(r + TOP, EDGE), BLOCK), :] = land[
                pl.ds(r, BLOCK), pl.ds(c * LANES, LANES)
            ].astype(jnp.float32)
        return carry

    lax.fori_loop(0, rows // BLOCK, wet_body, 0)
    for copy in field_loads:
        copy.wait()

    def lon_start(entries, buffers, slot):
        left_out, right_out, left_in, right_in = buffers

        def body(i, carry):
            r = pl.multiple_of(i * CHUNK, 8)
            lane = lax.broadcasted_iota(jnp.int32, (CHUNK, LANES), 1)
            left = right = None
            for k, (f, offset) in enumerate(entries):
                source = pl.ds(pl.multiple_of(r + (TOP + offset), 8), CHUNK)
                x = field[f, 0, source, :]
                y = field[f, tiles - 1, source, :]
                if k == 0:
                    left, right = x, y
                else:
                    shift = EDGE * k
                    left = jnp.where(lane >= shift, pltpu.roll(x, shift, 1), left)
                    right = jnp.where(lane < LANES - shift, pltpu.roll(y, LANES - shift, 1), right)
            left_out[pl.ds(r, CHUNK), :] = left
            right_out[pl.ds(r, CHUNK), :] = right
            return carry

        lax.fori_loop(0, left_out.shape[0] // CHUNK, body, 0)
        copies = tuple(
            pltpu.make_async_remote_copy(
                src_ref=source,
                dst_ref=target,
                send_sem=halo_send.at[slot + k],
                recv_sem=halo_recv.at[slot + k],
                device_id=device,
                device_id_type=MESH,
            )
            for k, (source, target, device) in enumerate(
                ((right_out, left_in, east), (left_out, right_in, west))
            )
        )
        for copy in copies:
            copy.start()
        return copies

    def lon_finish(entries, buffers, copies):
        left_in, right_in = buffers[2:]
        for copy in copies:
            copy.wait()

        def body(i, carry):
            r = pl.multiple_of(i * CHUNK, 8)
            lane = lax.broadcasted_iota(jnp.int32, (CHUNK, LANES), 1)
            x = right_in[pl.ds(r, CHUNK), :]
            y = left_in[pl.ds(r, CHUNK), :]
            for k, (f, offset) in enumerate(entries):
                a = pltpu.roll(x, LANES - EDGE * k, 1) if k else x
                b = pltpu.roll(y, EDGE * k, 1) if k else y
                target = pl.ds(pl.multiple_of(r + (TOP + offset), 8), CHUNK)
                field[f, halo, target, :] = jnp.where(
                    lane < EDGE, a, jnp.where(lane >= LANES - EDGE, b, 0.0)
                )
            return carry

        lax.fori_loop(0, left_in.shape[0] // CHUNK, body, 0)

    def lat_start(first, count, slot):
        def row_copy(source, target, at, device):
            return pltpu.make_async_remote_copy(
                src_ref=field.at[pl.ds(first, count), :, pl.ds(source, EDGE), :],
                dst_ref=field.at[pl.ds(first, count), :, pl.ds(target, EDGE), :],
                send_sem=halo_send.at[at],
                recv_sem=halo_recv.at[at],
                device_id=device,
                device_id_type=MESH,
            )

        to_north = row_copy(TOP, TOP + rows, slot, north)
        to_south = row_copy(TOP + rows - EDGE, TOP - EDGE, slot + 1, south)

        @pl.when(has_north)
        def _():
            to_north.start()

        @pl.when(has_south)
        def _():
            to_south.start()

        return to_north, to_south

    def lat_finish(to_north, to_south):
        @pl.when(has_north)
        def _():
            to_north.wait_send()
            to_south.wait_recv()

        @pl.when(has_south)
        def _():
            to_south.wait_send()
            to_north.wait_recv()

    wide_pack = (pack_left, pack_right, from_left, from_right)
    input_entries = [(f, 0) for f in range(3, FIELDS)]
    input_copies = lon_start(input_entries, wide_pack, 0)
    lon_finish(input_entries, wide_pack, input_copies)
    input_rows = lat_start(3, FIELDS - 3, 2)

    def sum_strip(c):
        def body(i, carry):
            strip(i, c).wait()
            total(i * CHUNK, CHUNK // EDGE, c, 1)
            return carry

        return body

    lax.fori_loop(0, pieces, sum_strip(0), 0)
    lax.fori_loop(0, pieces, sum_strip(tiles - 1), 0)
    for copy, r0 in zip(ends, (0, rows - EDGE)):
        copy.wait()
        total(r0, 1, 1, inner)
    short = rows // FOLD
    sum_pack = (sum_left, sum_right, sum_from_left, sum_from_right)
    sum_entries = [(f, g * short) for g in range(FOLD) for f in range(3)]
    sum_copies = lon_start(sum_entries, sum_pack, 4)
    lon_finish(sum_entries, sum_pack, sum_copies)
    sum_rows = lat_start(0, 3, 6)
    lat_finish(*input_rows)
    lat_finish(*sum_rows)

    bottom = TOP + rows - EDGE
    for k in range(2):
        derive(field, bottom + EDGE * k)
    sweep(field, outs, bottom, 2, lambda h: h, None, skip=(1,))

    middle(0).wait()
    total(EDGE, CHUNK // EDGE, 1, inner)
    count = CHUNK // EDGE + 2
    for k in range(count):
        derive(field, TOP - EDGE + EDGE * k)
    sweep(field, outs, TOP - EDGE, count, None, lambda h: EDGE - h, skip=(0,))

    def event(e, carry):
        middle(e).wait()
        r = EDGE + e * CHUNK
        total(r, CHUNK // EDGE, 1, inner)
        for k in range(CHUNK // EDGE):
            derive(field, TOP + r + EDGE * k)
        sweep(
            field,
            outs,
            TOP + r - EDGE,
            CHUNK // EDGE + 1,
            lambda h: EDGE - h,
            lambda h: EDGE - h,
        )
        return carry

    lax.fori_loop(1, events, event, 0)
    final.wait()
    total(rows - EDGE - FINAL, FINAL // EDGE, 1, inner)


def finish(*refs):
    sem = refs[-1]
    results = refs[6:11]
    field = refs[11]
    outs = refs[12:17]
    rows = outs[0].shape[0]
    cone = FINAL + 2 * EDGE
    done = rows - cone

    def write(k, r0, height, slot):
        at = pl.ds(r0, height)
        return pltpu.make_async_copy(outs[k].at[at], results[k].at[at], sem.at[slot])

    early = [write(k, 0, done, k) for k in range(5)]
    for copy in early:
        copy.start()
    start = TOP + done
    for k in range(FINAL // EDGE):
        derive(field, start + EDGE + EDGE * k)
    sweep(field, outs, start, cone // EDGE, lambda h: EDGE - h, lambda h: h)
    late = [write(k, done, cone, 5 + k) for k in range(5)]
    for copy in late:
        copy.start()
    for copy in early + late:
        copy.wait()


def shards(
    lat_count,
    lon_count,
    thickness,
    area,
    ridge_weight,
    cat_top,
    land_mask,
    velocity_u,
    velocity_v,
    stress_div,
    stress_ten,
    stress_shear,
    wind_x,
    wind_y,
    water_drag,
):
    cats, rows, cols = thickness.shape
    tiles = cols // LANES
    tall = rows + 2 * TOP
    f32 = jnp.float32
    events = (rows - 2 * EDGE - FINAL) // CHUNK
    pieces = rows // CHUNK
    slots = 2 * pieces + 3 + events
    anywhere = pl.BlockSpec(memory_space=pl.ANY)
    vmem = pl.BlockSpec(memory_space=pltpu.VMEM)
    state = (pltpu.VMEM((FIELDS, tiles + 1, tall, LANES), f32),) + tuple(
        pltpu.VMEM((rows, cols), f32) for _ in range(5)
    )
    results = pl.pallas_call(
        functools.partial(kernel, lat_count, lon_count),
        out_shape=state,
        in_specs=[pl.BlockSpec(memory_space=pltpu.SMEM)] + [anywhere] * 12,
        out_specs=(vmem,) * 6,
        scratch_shapes=[
            pltpu.VMEM((3, tiles, rows, LANES), f32),
            pltpu.VMEM((3, tiles, rows, LANES), f32),
            pltpu.VMEM((cats, rows, cols), thickness.dtype),
            pltpu.VMEM((cats, rows, cols), area.dtype),
            pltpu.VMEM((rows, cols), jnp.int32),
            pltpu.VMEM((rows, cols), jnp.int32),
            pltpu.VMEM((rows, LANES), f32),
            pltpu.VMEM((rows, LANES), f32),
            pltpu.VMEM((rows, LANES), f32),
            pltpu.VMEM((rows, LANES), f32),
            pltpu.VMEM((rows // FOLD, LANES), f32),
            pltpu.VMEM((rows // FOLD, LANES), f32),
            pltpu.VMEM((rows // FOLD, LANES), f32),
            pltpu.VMEM((rows // FOLD, LANES), f32),
            pltpu.SemaphoreType.DMA((13,)),
            pltpu.SemaphoreType.DMA((8 * tiles,)),
            pltpu.SemaphoreType.DMA((slots,)),
            pltpu.SemaphoreType.DMA((slots,)),
            pltpu.SemaphoreType.DMA((8,)),
            pltpu.SemaphoreType.DMA((8,)),
        ],
        compiler_params=pltpu.CompilerParams(
            collective_id=0, has_side_effects=True, vmem_limit_bytes=44 * 2**20
        ),
        name="ice",
    )(
        ridge_weight,
        thickness,
        area,
        cat_top,
        land_mask,
        velocity_u,
        velocity_v,
        stress_div,
        stress_ten,
        stress_shear,
        wind_x,
        wind_y,
        water_drag,
    )
    return pl.pallas_call(
        finish,
        out_shape=tuple(jax.ShapeDtypeStruct((rows, cols), f32) for _ in range(5)) + state,
        in_specs=[vmem] * 6,
        out_specs=(anywhere,) * 5 + (vmem,) * 6,
        input_output_aliases={k: 5 + k for k in range(6)},
        scratch_shapes=[pltpu.SemaphoreType.DMA((10,))],
        compiler_params=pltpu.CompilerParams(vmem_limit_bytes=4 * 2**20),
        name="finish",
    )(*results)[:5]


def solution(mesh):
    body = functools.partial(shards, mesh.shape["lat"], mesh.shape["lon"])
    plane = P("lat", "lon")
    return jax.shard_map(
        body,
        mesh=mesh,
        in_specs=(P("cat", "lat", "lon"), P("cat", "lat", "lon"), P("cat")) + (plane,) * 10,
        out_specs=(plane,) * 5,
        check_vma=False,
    )
```

```python
import functools

import jax
import jax.numpy as jnp
from jax import lax
from jax.experimental import pallas as pl
from jax.experimental.pallas import tpu as pltpu
from jax.sharding import PartitionSpec as P

SUB = 4
LANES = 128
EDGE = 8
BLOCK = 16
CHUNK = 32
TAIL = (16, 16)
FINAL = 16
TOP = 16
FOLD = 4
MESH = pl.DeviceIdType.MESH

FS, FM, FC, FD, FX, FY, FW, FU, FV, FA, FB, FT = range(12)
FIELDS = 12
THIRD = 1.0 / 3.0


def read(field, f, c, r, shift=0):
    if shift == 0:
        return field[f, c, pl.ds(pl.multiple_of(r, EDGE), EDGE), :]
    near = field.at[f, c, pl.ds(pl.multiple_of(r - EDGE, EDGE), 3 * EDGE)]
    return near[EDGE + shift : 2 * EDGE + shift, :]


def put(ref, value, mask):
    if mask is None:
        ref[...] = value
    else:
        pltpu.store(ref, value, mask=mask)


def along(x, lane):
    tiles = len(x)
    ahead = [pltpu.roll(a, LANES - 1, 1) for a in x]
    behind = [pltpu.roll(a, 1, 1) for a in x]
    return [
        jnp.where(lane == LANES - 1, ahead[(c + 1) % tiles], ahead[c])
        - jnp.where(lane == 0, behind[c - 1], behind[c])
        for c in range(tiles)
    ]


def derive(field, r):
    tiles = field.shape[1]
    at = pl.ds(pl.multiple_of(r, EDGE), EDGE)
    for c in range(tiles):
        wet = field[FW, c, at, :]
        mass = field[FM, c, at, :]
        ratio = wet / (mass + field[FD, c, at, :] + 1.0 - wet)
        force = field[FC, c, at, :] * ratio
        field[FS, c, at, :] = (2.0 * THIRD) * wet * field[FS, c, at, :]
        field[FM, c, at, :] = mass * ratio
        field[FD, c, at, :] = 0.25 * ratio
        field[FX, c, at, :] = force * field[FX, c, at, :]
        field[FY, c, at, :] = force * field[FY, c, at, :]
        field[FW, c, at, :] = THIRD * wet
        first = field[FA, c, at, :]
        second = field[FB, c, at, :]
        field[FA, c, at, :] = first + second
        field[FB, c, at, :] = first - second
        field[FT, c, at, :] = 2.0 * field[FT, c, at, :]


def stress(field, outs, r, mask, lane):
    tiles = field.shape[1]
    at = pl.ds(pl.multiple_of(r, EDGE), EDGE)
    dxu = along([field[FU, c, at, :] for c in range(tiles)], lane)
    dxv = along([field[FV, c, at, :] for c in range(tiles)], lane)
    for c in range(tiles):
        dyu = read(field, FU, c, r, 1) - read(field, FU, c, r, -1)
        dyv = read(field, FV, c, r, 1) - read(field, FV, c, r, -1)
        div = dxu[c] + dyv
        ten = dxu[c] - dyv
        shr = dyu + dxv[c]
        inverse = lax.rsqrt(div * div + 0.25 * (ten * ten + shr * shr) + 0.01)
        power = field[FS, c, at, :]
        keep = field[FW, c, at, :]
        gain = power * inverse
        p = gain * div - power
        q = (0.25 * gain) * ten
        a = keep * field[FA, c, at, :] + (p + q)
        b = keep * field[FB, c, at, :] + (p - q)
        s = keep * field[FT, c, at, :] + (0.5 * gain) * shr
        put(field.at[FA, c, at], a, mask)
        put(field.at[FB, c, at], b, mask)
        put(field.at[FT, c, at], s, mask)
        if outs is not None and c < tiles - 1:
            spot = (pl.ds(pl.multiple_of(r - TOP, EDGE), EDGE), pl.ds(c * LANES, LANES))
            put(outs[2].at[spot], 0.5 * (a + b), mask)
            put(outs[3].at[spot], 0.5 * (a - b), mask)
            put(outs[4].at[spot], 0.5 * s, mask)


def motion(field, outs, r, mask, lane):
    tiles = field.shape[1]
    at = pl.ds(pl.multiple_of(r, EDGE), EDGE)
    dxa = along([field[FA, c, at, :] for c in range(tiles)], lane)
    dxt = along([field[FT, c, at, :] for c in range(tiles)], lane)
    for c in range(tiles):
        fx = dxa[c] + (read(field, FT, c, r, 1) - read(field, FT, c, r, -1))
        fy = dxt[c] + (read(field, FB, c, r, 1) - read(field, FB, c, r, -1))
        u = field[FU, c, at, :]
        v = field[FV, c, at, :]
        inertia = field[FM, c, at, :]
        ratio = field[FD, c, at, :]
        new_u = inertia * (u + 0.5 * v) + ratio * fx + field[FX, c, at, :]
        new_v = inertia * (v - 0.5 * u) + ratio * fy + field[FY, c, at, :]
        put(field.at[FU, c, at], new_u, mask)
        put(field.at[FV, c, at], new_v, mask)
        if outs is not None and c < tiles - 1:
            spot = (pl.ds(pl.multiple_of(r - TOP, EDGE), EDGE), pl.ds(c * LANES, LANES))
            put(outs[0].at[spot], new_u, mask)
            put(outs[1].at[spot], new_v, mask)


def sweep(field, outs, start, count, head, tail, skip=(), between=None):
    lane = lax.broadcasted_iota(jnp.int32, (EDGE, LANES), 1)
    line = lax.broadcasted_iota(jnp.int32, (EDGE, LANES), 0)

    def half(step, h, emit):
        for k in range(count):
            mask = None
            if k == 0 and head is not None:
                mask = line >= head(h)
            if k == count - 1 and tail is not None:
                mask = line < tail(h)
            step(field, outs if emit and k not in skip else None, start + EDGE * k, mask, lane)

    def cycle(t, carry):
        half(stress, 2 * t, False)
        half(motion, 2 * t + 1, False)
        return carry

    lax.fori_loop(0, SUB - 1, cycle, 0)
    half(stress, 2 * SUB - 2, True)
    if between is not None:
        between()
    half(motion, 2 * SUB - 1, True)


def kernel(
    lat_count,
    lon_count,
    weight_hbm,
    thick_hbm,
    area_hbm,
    top_hbm,
    land_hbm,
    u_hbm,
    v_hbm,
    s1_hbm,
    s2_hbm,
    s3_hbm,
    wx_hbm,
    wy_hbm,
    drag_hbm,
    field,
    out_u,
    out_v,
    out_1,
    out_2,
    out_3,
    weight,
    own,
    other,
    thick,
    area,
    top,
    land,
    pack_left,
    pack_right,
    from_left,
    from_right,
    sum_left,
    sum_right,
    sum_from_left,
    sum_from_right,
    load_sem,
    field_sem,
    x_send,
    x_recv,
    halo_send,
    halo_recv,
    ready,
):
    outs = (out_u, out_v, out_1, out_2, out_3)
    cats, rows, cols = thick.shape
    tiles = cols // LANES
    halo = tiles
    inner = tiles - 2
    last = cols - LANES
    pieces = rows // CHUNK
    events = (rows - 2 * EDGE - FINAL - sum(TAIL)) // CHUNK
    my_cat = lax.axis_index("cat")
    my_lat = lax.axis_index("lat")
    my_lon = lax.axis_index("lon")
    partner = {"cat": 1 - my_cat}
    west = {"lon": lax.rem(my_lon + lon_count - 1, lon_count)}
    east = {"lon": lax.rem(my_lon + 1, lon_count)}
    north = {"lat": my_lat - 1}
    south = {"lat": my_lat + 1}
    has_north = my_lat > 0
    has_south = my_lat < lat_count - 1

    early = lax.rem(my_lat + my_lon, 2) == 0
    late = jnp.logical_not(early)
    around = 2 + has_north.astype(jnp.int32) + has_south.astype(jnp.int32)
    barrier = pltpu.get_barrier_semaphore()
    pl.semaphore_signal(barrier, inc=1, device_id=partner, device_id_type=MESH)

    def greet(semaphore, when):
        for device, there in ((west, when), (east, when), (north, when & has_north), (south, when & has_south)):

            @pl.when(there)
            def _():
                pl.semaphore_signal(semaphore, inc=1, device_id=device, device_id_type=MESH)

    greet(barrier, early)
    weight_load = pltpu.make_async_copy(weight_hbm, weight, load_sem.at[13])
    weight_load.start()

    groups = (
        (0, CHUNK, 0, LANES),
        (CHUNK, rows - CHUNK, 0, LANES),
        (0, rows, last, LANES),
        (0, rows, LANES, cols - 2 * LANES),
    )
    loads = []
    for k, (r0, height, c0, w) in enumerate(groups):
        spot = (pl.ds(r0, height), pl.ds(c0, w))
        group = (
            pltpu.make_async_copy(top_hbm.at[spot], top.at[spot], load_sem.at[3 * k]),
            pltpu.make_async_copy(
                thick_hbm.at[(slice(None),) + spot], thick.at[(slice(None),) + spot], load_sem.at[3 * k + 1]
            ),
            pltpu.make_async_copy(
                area_hbm.at[(slice(None),) + spot], area.at[(slice(None),) + spot], load_sem.at[3 * k + 2]
            ),
        )
        for copy in group:
            copy.start()
        loads.append(group)

    base = my_cat * cats

    def partial(r0, count, c0, w):
        def body(i, carry):
            r = pl.multiple_of(r0 + i * BLOCK, BLOCK)
            at = pl.ds(r, BLOCK)
            for c in range(c0, c0 + w):
                lanes = pl.ds(c * LANES, LANES)
                limit = top[at, lanes] - base
                strength = mass = conc = jnp.zeros((BLOCK, LANES), jnp.float32)
                for n in range(cats):
                    height = thick[n, at, lanes].astype(jnp.float32)
                    cover = jnp.where(limit > n, area[n, at, lanes].astype(jnp.float32), 0.0)
                    volume = cover * height
                    conc = conc + cover
                    mass = mass + volume
                    strength = strength + weight[n] * (volume * height)
                own[0, c, at, :] = strength
                own[1, c, at, :] = mass
                own[2, c, at, :] = conc
            return carry

        lax.fori_loop(0, count, body, 0)

    def exchange(slot, r0, height, c0, w):
        part = (pl.ds(0, 3), pl.ds(c0, w), pl.ds(r0, height))
        return pltpu.make_async_remote_copy(
            src_ref=own.at[part],
            dst_ref=other.at[part],
            send_sem=x_send.at[slot],
            recv_sem=x_recv.at[slot],
            device_id=partner,
            device_id_type=MESH,
        )

    def strip(i, c):
        return exchange((pieces if c else 0) + i, pl.multiple_of(i * CHUNK, CHUNK), CHUNK, c, 1)

    ends = (
        exchange(2 * pieces, 0, EDGE, 1, inner),
        exchange(2 * pieces + 1, rows - EDGE, EDGE, 1, inner),
    )
    final = exchange(2 * pieces + 2, rows - EDGE - FINAL, FINAL, 1, inner)

    def middle(e):
        return exchange(2 * pieces + 3 + e, pl.multiple_of(EDGE + e * CHUNK, EDGE), CHUNK, 1, inner)

    tail_rows = [EDGE + events * CHUNK + sum(TAIL[:k]) for k in range(len(TAIL))]
    tail = [
        exchange(2 * pieces + 3 + events + k, r0, height, 1, inner)
        for k, (r0, height) in enumerate(zip(tail_rows, TAIL))
    ]

    def total(r0, count, c0, w):
        for k in range(count):
            r = pl.multiple_of(r0 + k * EDGE, EDGE)
            at = pl.ds(r, EDGE)
            target = pl.ds(pl.multiple_of(r + TOP, EDGE), EDGE)
            for f in range(3):
                for c in range(c0, c0 + w):
                    field[f, c, target, :] = own[f, c, at, :] + other[f, c, at, :]

    weight_load.wait()
    for copy in loads[0]:
        copy.wait()
    partial(0, CHUNK // BLOCK, 0, 1)
    pl.semaphore_wait(barrier, jnp.where(early, 1, 1 + around))
    strip(0, 0).start()
    greet(ready, late)

    def send_strip(c):
        def body(i, carry):
            partial(i * CHUNK, CHUNK // BLOCK, c, 1)
            strip(i, c).start()
            return carry

        return body

    for copy in loads[1]:
        copy.wait()
    lax.fori_loop(1, pieces, send_strip(0), 0)

    land_load = pltpu.make_async_copy(land_hbm, land, load_sem.at[12])
    land_load.start()
    field_loads = []
    for k, (f, ref) in enumerate(
        (
            (FU, u_hbm),
            (FV, v_hbm),
            (FA, s1_hbm),
            (FB, s2_hbm),
            (FT, s3_hbm),
            (FX, wx_hbm),
            (FY, wy_hbm),
            (FD, drag_hbm),
        )
    ):
        for c in range(tiles):
            copy = pltpu.make_async_copy(
                ref.at[:, pl.ds(c * LANES, LANES)],
                field.at[f, c, pl.ds(TOP, rows)],
                field_sem.at[k * tiles + c],
            )
            copy.start()
            field_loads.append(copy)

    @pl.when(jnp.logical_not(has_north))
    def _():
        field[:, :, pl.ds(TOP - EDGE, EDGE), :] = jnp.zeros((FIELDS, tiles + 1, EDGE, LANES), jnp.float32)

    @pl.when(jnp.logical_not(has_south))
    def _():
        field[:, :, pl.ds(TOP + rows, EDGE), :] = jnp.zeros((FIELDS, tiles + 1, EDGE, LANES), jnp.float32)

    for copy in loads[2]:
        copy.wait()
    lax.fori_loop(0, pieces, send_strip(tiles - 1), 0)
    for copy in loads[3]:
        copy.wait()
    partial(0, 1, 1, inner)
    ends[0].start()
    partial(rows - BLOCK, 1, 1, inner)
    ends[1].start()

    def send_middle(e, carry):
        partial(BLOCK + e * CHUNK, CHUNK // BLOCK, 1, inner)
        middle(e).start()
        return carry

    lax.fori_loop(0, events, send_middle, 0)
    reached = BLOCK + events * CHUNK
    partial(reached, (rows - BLOCK - reached) // BLOCK, 1, inner)
    for copy in tail:
        copy.start()
    final.start()

    land_load.wait()

    def wet_body(i, carry):
        r = pl.multiple_of(i * BLOCK, BLOCK)
        for c in range(tiles):
            field[FW, c, pl.ds(pl.multiple_of(r + TOP, EDGE), BLOCK), :] = land[
                pl.ds(r, BLOCK), pl.ds(c * LANES, LANES)
            ].astype(jnp.float32)
        return carry

    lax.fori_loop(0, rows // BLOCK, wet_body, 0)
    for copy in field_loads:
        copy.wait()

    def lon_start(entries, buffers, slot):
        left_out, right_out, left_in, right_in = buffers

        def body(i, carry):
            r = pl.multiple_of(i * CHUNK, 8)
            lane = lax.broadcasted_iota(jnp.int32, (CHUNK, LANES), 1)
            left = right = None
            for k, (f, offset) in enumerate(entries):
                source = pl.ds(pl.multiple_of(r + (TOP + offset), 8), CHUNK)
                x = field[f, 0, source, :]
                y = field[f, tiles - 1, source, :]
                if k == 0:
                    left, right = x, y
                else:
                    shift = EDGE * k
                    left = jnp.where(lane >= shift, pltpu.roll(x, shift, 1), left)
                    right = jnp.where(lane < LANES - shift, pltpu.roll(y, LANES - shift, 1), right)
            left_out[pl.ds(r, CHUNK), :] = left
            right_out[pl.ds(r, CHUNK), :] = right
            return carry

        lax.fori_loop(0, left_out.shape[0] // CHUNK, body, 0)
        copies = tuple(
            pltpu.make_async_remote_copy(
                src_ref=source,
                dst_ref=target,
                send_sem=halo_send.at[slot + k],
                recv_sem=halo_recv.at[slot + k],
                device_id=device,
                device_id_type=MESH,
            )
            for k, (source, target, device) in enumerate(
                ((right_out, left_in, east), (left_out, right_in, west))
            )
        )
        for copy in copies:
            copy.start()
        return copies

    def lon_finish(entries, buffers, copies):
        left_in, right_in = buffers[2:]
        for copy in copies:
            copy.wait()

        def body(i, carry):
            r = pl.multiple_of(i * CHUNK, 8)
            lane = lax.broadcasted_iota(jnp.int32, (CHUNK, LANES), 1)
            x = right_in[pl.ds(r, CHUNK), :]
            y = left_in[pl.ds(r, CHUNK), :]
            for k, (f, offset) in enumerate(entries):
                a = pltpu.roll(x, LANES - EDGE * k, 1) if k else x
                b = pltpu.roll(y, EDGE * k, 1) if k else y
                target = pl.ds(pl.multiple_of(r + (TOP + offset), 8), CHUNK)
                field[f, halo, target, :] = jnp.where(
                    lane < EDGE, a, jnp.where(lane >= LANES - EDGE, b, 0.0)
                )
            return carry

        lax.fori_loop(0, left_in.shape[0] // CHUNK, body, 0)

    def lat_start(first, count, slot):
        def row_copy(source, target, at, device):
            return pltpu.make_async_remote_copy(
                src_ref=field.at[pl.ds(first, count), :, pl.ds(source, EDGE), :],
                dst_ref=field.at[pl.ds(first, count), :, pl.ds(target, EDGE), :],
                send_sem=halo_send.at[at],
                recv_sem=halo_recv.at[at],
                device_id=device,
                device_id_type=MESH,
            )

        to_north = row_copy(TOP, TOP + rows, slot, north)
        to_south = row_copy(TOP + rows - EDGE, TOP - EDGE, slot + 1, south)

        @pl.when(has_north)
        def _():
            to_north.start()

        @pl.when(has_south)
        def _():
            to_south.start()

        return to_north, to_south

    def lat_finish(to_north, to_south):
        @pl.when(has_north)
        def _():
            to_north.wait_send()
            to_south.wait_recv()

        @pl.when(has_south)
        def _():
            to_south.wait_send()
            to_north.wait_recv()

    wide_pack = (pack_left, pack_right, from_left, from_right)
    input_entries = [(f, 0) for f in range(3, FIELDS)]

    @pl.when(early)
    def _():
        pl.semaphore_wait(ready, around)

    input_copies = lon_start(input_entries, wide_pack, 0)
    lon_finish(input_entries, wide_pack, input_copies)
    input_rows = lat_start(3, FIELDS - 3, 2)

    def sum_strip(c):
        def body(i, carry):
            strip(i, c).wait()
            total(i * CHUNK, CHUNK // EDGE, c, 1)
            return carry

        return body

    lax.fori_loop(0, pieces, sum_strip(0), 0)
    lax.fori_loop(0, pieces, sum_strip(tiles - 1), 0)
    for copy, r0 in zip(ends, (0, rows - EDGE)):
        copy.wait()
        total(r0, 1, 1, inner)
    short = rows // FOLD
    sum_pack = (sum_left, sum_right, sum_from_left, sum_from_right)
    sum_entries = [(f, g * short) for g in range(FOLD) for f in range(3)]
    sum_copies = lon_start(sum_entries, sum_pack, 4)
    lon_finish(sum_entries, sum_pack, sum_copies)
    sum_rows = lat_start(0, 3, 6)
    lat_finish(*input_rows)
    lat_finish(*sum_rows)

    bottom = TOP + rows - EDGE
    for k in range(2):
        derive(field, bottom + EDGE * k)
    sweep(field, outs, bottom, 2, lambda h: h, None, skip=(1,))

    middle(0).wait()
    total(EDGE, CHUNK // EDGE, 1, inner)
    count = CHUNK // EDGE + 2
    for k in range(count):
        derive(field, TOP - EDGE + EDGE * k)
    sweep(field, outs, TOP - EDGE, count, None, lambda h: EDGE - h, skip=(0,))

    def advance(r, height):
        total(r, height // EDGE, 1, inner)
        for k in range(height // EDGE):
            derive(field, TOP + r + EDGE * k)
        sweep(
            field,
            outs,
            TOP + r - EDGE,
            height // EDGE + 1,
            lambda h: EDGE - h,
            lambda h: EDGE - h,
        )

    def event(e, carry):
        middle(e).wait()
        advance(EDGE + e * CHUNK, CHUNK)
        return carry

    lax.fori_loop(1, events, event, 0)
    for copy, r0, height in zip(tail, tail_rows, TAIL):
        copy.wait()
        advance(r0, height)
    final.wait()
    total(rows - EDGE - FINAL, FINAL // EDGE, 1, inner)


def finish(*refs):
    sem = refs[-1]
    results = refs[6:11]
    field = refs[11]
    outs = refs[12:17]
    rows = outs[0].shape[0]
    cone = FINAL + 2 * EDGE
    done = rows - cone

    def write(k, r0, height, slot):
        at = pl.ds(r0, height)
        return pltpu.make_async_copy(outs[k].at[at], results[k].at[at], sem.at[slot])

    early = [write(k, 0, done, k) for k in range(5)]
    for copy in early:
        copy.start()
    start = TOP + done
    for k in range(FINAL // EDGE):
        derive(field, start + EDGE + EDGE * k)
    late = [write(k, done, cone, 5 + k) for k in range(5)]

    def write_stress():
        for copy in late[2:]:
            copy.start()

    sweep(field, outs, start, cone // EDGE, lambda h: EDGE - h, lambda h: h, between=write_stress)
    for copy in late[:2]:
        copy.start()
    for copy in early + late:
        copy.wait()


def shards(
    lat_count,
    lon_count,
    thickness,
    area,
    ridge_weight,
    cat_top,
    land_mask,
    velocity_u,
    velocity_v,
    stress_div,
    stress_ten,
    stress_shear,
    wind_x,
    wind_y,
    water_drag,
):
    cats, rows, cols = thickness.shape
    tiles = cols // LANES
    tall = rows + 2 * TOP
    f32 = jnp.float32
    events = (rows - 2 * EDGE - FINAL - sum(TAIL)) // CHUNK
    pieces = rows // CHUNK
    slots = 2 * pieces + 3 + events + len(TAIL)
    anywhere = pl.BlockSpec(memory_space=pl.ANY)
    vmem = pl.BlockSpec(memory_space=pltpu.VMEM)
    state = (pltpu.VMEM((FIELDS, tiles + 1, tall, LANES), f32),) + tuple(
        pltpu.VMEM((rows, cols), f32) for _ in range(5)
    )
    results = pl.pallas_call(
        functools.partial(kernel, lat_count, lon_count),
        out_shape=state,
        in_specs=[anywhere] * 13,
        out_specs=(vmem,) * 6,
        scratch_shapes=[
            pltpu.SMEM((cats,), f32),
            pltpu.VMEM((3, tiles, rows, LANES), f32),
            pltpu.VMEM((3, tiles, rows, LANES), f32),
            pltpu.VMEM((cats, rows, cols), thickness.dtype),
            pltpu.VMEM((cats, rows, cols), area.dtype),
            pltpu.VMEM((rows, cols), jnp.int32),
            pltpu.VMEM((rows, cols), jnp.int32),
            pltpu.VMEM((rows, LANES), f32),
            pltpu.VMEM((rows, LANES), f32),
            pltpu.VMEM((rows, LANES), f32),
            pltpu.VMEM((rows, LANES), f32),
            pltpu.VMEM((rows // FOLD, LANES), f32),
            pltpu.VMEM((rows // FOLD, LANES), f32),
            pltpu.VMEM((rows // FOLD, LANES), f32),
            pltpu.VMEM((rows // FOLD, LANES), f32),
            pltpu.SemaphoreType.DMA((14,)),
            pltpu.SemaphoreType.DMA((8 * tiles,)),
            pltpu.SemaphoreType.DMA((slots,)),
            pltpu.SemaphoreType.DMA((slots,)),
            pltpu.SemaphoreType.DMA((8,)),
            pltpu.SemaphoreType.DMA((8,)),
            pltpu.SemaphoreType.REGULAR,
        ],
        compiler_params=pltpu.CompilerParams(
            collective_id=0, has_side_effects=True, vmem_limit_bytes=44 * 2**20
        ),
        name="ice",
    )(
        ridge_weight,
        thickness,
        area,
        cat_top,
        land_mask,
        velocity_u,
        velocity_v,
        stress_div,
        stress_ten,
        stress_shear,
        wind_x,
        wind_y,
        water_drag,
    )
    return pl.pallas_call(
        finish,
        out_shape=tuple(jax.ShapeDtypeStruct((rows, cols), f32) for _ in range(5)) + state,
        in_specs=[vmem] * 6,
        out_specs=(anywhere,) * 5 + (vmem,) * 6,
        input_output_aliases={k: 5 + k for k in range(6)},
        scratch_shapes=[pltpu.SemaphoreType.DMA((10,))],
        compiler_params=pltpu.CompilerParams(vmem_limit_bytes=4 * 2**20),
        name="finish",
    )(*results)[:5]


def solution(mesh):
    body = functools.partial(shards, mesh.shape["lat"], mesh.shape["lon"])
    plane = P("lat", "lon")
    return jax.shard_map(
        body,
        mesh=mesh,
        in_specs=(P("cat", "lat", "lon"), P("cat", "lat", "lon"), P("cat")) + (plane,) * 10,
        out_specs=(plane,) * 5,
        check_vma=False,
    )
```

```python
import functools

import jax
import jax.numpy as jnp
from jax import lax
from jax.experimental import pallas as pl
from jax.experimental.pallas import tpu as pltpu
from jax.sharding import PartitionSpec as P

SUB = 4
LANES = 128
EDGE = 8
BLOCK = 16
CHUNK = 32
TAIL = (16, 16)
FINAL = 16
TOP = 16
LEFT = (16, 48, 64, 128)
RIGHT = (128, 128)
PAIR = 1
FOLD = 4
MESH = pl.DeviceIdType.MESH

FS, FM, FC, FD, FX, FY, FW, FU, FV, FA, FB, FT = range(12)
FIELDS = 12
THIRD = 1.0 / 3.0


def read(field, f, c, r, shift=0):
    if shift == 0:
        return field[f, c, pl.ds(pl.multiple_of(r, EDGE), EDGE), :]
    near = field.at[f, c, pl.ds(pl.multiple_of(r - EDGE, EDGE), 3 * EDGE)]
    return near[EDGE + shift : 2 * EDGE + shift, :]


def put(ref, value, mask):
    if mask is None:
        ref[...] = value
    else:
        pltpu.store(ref, value, mask=mask)


def along(x, lane):
    tiles = len(x)
    ahead = [pltpu.roll(a, LANES - 1, 1) for a in x]
    behind = [pltpu.roll(a, 1, 1) for a in x]
    return [
        jnp.where(lane == LANES - 1, ahead[(c + 1) % tiles], ahead[c])
        - jnp.where(lane == 0, behind[c - 1], behind[c])
        for c in range(tiles)
    ]


def derive(field, r):
    tiles = field.shape[1]
    at = pl.ds(pl.multiple_of(r, EDGE), EDGE)
    for c in range(tiles):
        wet = field[FW, c, at, :]
        mass = field[FM, c, at, :]
        ratio = wet / (mass + field[FD, c, at, :] + 1.0 - wet)
        force = field[FC, c, at, :] * ratio
        field[FS, c, at, :] = (2.0 * THIRD) * wet * field[FS, c, at, :]
        field[FM, c, at, :] = mass * ratio
        field[FD, c, at, :] = 0.25 * ratio
        field[FX, c, at, :] = force * field[FX, c, at, :]
        field[FY, c, at, :] = force * field[FY, c, at, :]
        field[FW, c, at, :] = THIRD * wet
        first = field[FA, c, at, :]
        second = field[FB, c, at, :]
        field[FA, c, at, :] = first + second
        field[FB, c, at, :] = first - second
        field[FT, c, at, :] = 2.0 * field[FT, c, at, :]


def stress(field, outs, r, mask, lane):
    tiles = field.shape[1]
    at = pl.ds(pl.multiple_of(r, EDGE), EDGE)
    dxu = along([field[FU, c, at, :] for c in range(tiles)], lane)
    dxv = along([field[FV, c, at, :] for c in range(tiles)], lane)
    for c in range(tiles):
        dyu = read(field, FU, c, r, 1) - read(field, FU, c, r, -1)
        dyv = read(field, FV, c, r, 1) - read(field, FV, c, r, -1)
        div = dxu[c] + dyv
        ten = dxu[c] - dyv
        shr = dyu + dxv[c]
        inverse = lax.rsqrt(div * div + 0.25 * (ten * ten + shr * shr) + 0.01)
        power = field[FS, c, at, :]
        keep = field[FW, c, at, :]
        gain = power * inverse
        p = gain * div - power
        q = (0.25 * gain) * ten
        a = keep * field[FA, c, at, :] + (p + q)
        b = keep * field[FB, c, at, :] + (p - q)
        s = keep * field[FT, c, at, :] + (0.5 * gain) * shr
        put(field.at[FA, c, at], a, mask)
        put(field.at[FB, c, at], b, mask)
        put(field.at[FT, c, at], s, mask)
        if outs is not None and c < tiles - 1:
            spot = (pl.ds(pl.multiple_of(r - TOP, EDGE), EDGE), pl.ds(c * LANES, LANES))
            put(outs[2].at[spot], 0.5 * (a + b), mask)
            put(outs[3].at[spot], 0.5 * (a - b), mask)
            put(outs[4].at[spot], 0.5 * s, mask)


def motion(field, outs, r, mask, lane):
    tiles = field.shape[1]
    at = pl.ds(pl.multiple_of(r, EDGE), EDGE)
    dxa = along([field[FA, c, at, :] for c in range(tiles)], lane)
    dxt = along([field[FT, c, at, :] for c in range(tiles)], lane)
    for c in range(tiles):
        fx = dxa[c] + (read(field, FT, c, r, 1) - read(field, FT, c, r, -1))
        fy = dxt[c] + (read(field, FB, c, r, 1) - read(field, FB, c, r, -1))
        u = field[FU, c, at, :]
        v = field[FV, c, at, :]
        inertia = field[FM, c, at, :]
        ratio = field[FD, c, at, :]
        new_u = inertia * (u + 0.5 * v) + ratio * fx + field[FX, c, at, :]
        new_v = inertia * (v - 0.5 * u) + ratio * fy + field[FY, c, at, :]
        put(field.at[FU, c, at], new_u, mask)
        put(field.at[FV, c, at], new_v, mask)
        if outs is not None and c < tiles - 1:
            spot = (pl.ds(pl.multiple_of(r - TOP, EDGE), EDGE), pl.ds(c * LANES, LANES))
            put(outs[0].at[spot], new_u, mask)
            put(outs[1].at[spot], new_v, mask)


def sweep(field, outs, start, count, head, tail, skip=(), between=None, unroll=False):
    lane = lax.broadcasted_iota(jnp.int32, (EDGE, LANES), 1)
    line = lax.broadcasted_iota(jnp.int32, (EDGE, LANES), 0)

    def half(step, h, emit):
        for k in range(count):
            mask = None
            if k == 0 and head is not None:
                mask = line >= head(h)
            if k == count - 1 and tail is not None:
                mask = line < tail(h)
            step(field, outs if emit and k not in skip else None, start + EDGE * k, mask, lane)

    def cycle(t, carry):
        half(stress, 2 * t, False)
        half(motion, 2 * t + 1, False)
        return carry

    if unroll:
        for t in range(SUB - 1):
            cycle(t, 0)
    else:
        lax.fori_loop(0, SUB - 1, cycle, 0)
    half(stress, 2 * SUB - 2, True)
    if between is not None:
        between()
    half(motion, 2 * SUB - 1, True)


def kernel(
    lat_count,
    lon_count,
    weight_hbm,
    thick_hbm,
    area_hbm,
    top_hbm,
    land_hbm,
    u_hbm,
    v_hbm,
    s1_hbm,
    s2_hbm,
    s3_hbm,
    wx_hbm,
    wy_hbm,
    drag_hbm,
    field,
    out_u,
    out_v,
    out_1,
    out_2,
    out_3,
    weight,
    own,
    other,
    thick,
    area,
    top,
    land,
    pack_left,
    pack_right,
    from_left,
    from_right,
    sum_left,
    sum_right,
    sum_from_left,
    sum_from_right,
    load_sem,
    field_sem,
    x_send,
    x_recv,
    halo_send,
    halo_recv,
    ready,
    token,
):
    outs = (out_u, out_v, out_1, out_2, out_3)
    cats, rows, cols = thick.shape
    tiles = cols // LANES
    halo = tiles
    inner = tiles - 2
    last = cols - LANES
    events = (rows - 2 * EDGE - FINAL - sum(TAIL)) // CHUNK
    my_cat = lax.axis_index("cat")
    my_lat = lax.axis_index("lat")
    my_lon = lax.axis_index("lon")
    partner = {"cat": 1 - my_cat}
    west = {"lon": lax.rem(my_lon + lon_count - 1, lon_count)}
    east = {"lon": lax.rem(my_lon + 1, lon_count)}
    north = {"lat": my_lat - 1}
    south = {"lat": my_lat + 1}
    has_north = my_lat > 0
    has_south = my_lat < lat_count - 1


    groups = (
        (0, LEFT[0], 0, LANES),
        (LEFT[0], LEFT[1], 0, LANES),
        (LEFT[0] + LEFT[1], rows - LEFT[0] - LEFT[1], 0, LANES),
        (0, rows, last, LANES),
        (0, rows, LANES, cols - 2 * LANES),
    )
    loads = []
    for k, (r0, height, c0, w) in enumerate(groups):
        spot = (pl.ds(r0, height), pl.ds(c0, w))
        group = (
            pltpu.make_async_copy(top_hbm.at[spot], top.at[spot], load_sem.at[3 * k]),
            pltpu.make_async_copy(
                thick_hbm.at[(slice(None),) + spot], thick.at[(slice(None),) + spot], load_sem.at[3 * k + 1]
            ),
            pltpu.make_async_copy(
                area_hbm.at[(slice(None),) + spot], area.at[(slice(None),) + spot], load_sem.at[3 * k + 2]
            ),
        )
        loads.append(group)

    def load(*which):
        for k in which:
            for copy in loads[k]:
                copy.start()

    def loaded(k):
        for copy in loads[k]:
            copy.wait()

    load(0)
    weight_load = pltpu.make_async_copy(weight_hbm, weight, load_sem.at[16])
    weight_load.start()
    load(1)

    has_west = my_lon > 0
    has_east = my_lon < lon_count - 1
    before = 1 + has_north.astype(jnp.int32) + has_west.astype(jnp.int32)
    after = has_south.astype(jnp.int32) + has_east.astype(jnp.int32)
    barrier = pltpu.get_barrier_semaphore()
    pl.semaphore_signal(barrier, inc=1, device_id=partner, device_id_type=MESH)

    def greet(semaphore, *devices):
        for device, there in devices:

            @pl.when(there)
            def _():
                pl.semaphore_signal(semaphore, inc=1, device_id=device, device_id_type=MESH)

    greet(barrier, (south, has_south), (east, has_east))
    base = my_cat * cats

    def partial(r0, count, c0, w):
        def body(i, carry):
            r = pl.multiple_of(r0 + i * BLOCK, BLOCK)
            at = pl.ds(r, BLOCK)
            for c in range(c0, c0 + w):
                lanes = pl.ds(c * LANES, LANES)
                limit = top[at, lanes] - base
                strength = mass = conc = jnp.zeros((BLOCK, LANES), jnp.float32)
                for n in range(cats):
                    height = thick[n, at, lanes].astype(jnp.float32)
                    cover = jnp.where(limit > n, area[n, at, lanes].astype(jnp.float32), 0.0)
                    volume = cover * height
                    conc = conc + cover
                    mass = mass + volume
                    strength = strength + weight[n] * (volume * height)
                own[0, c, at, :] = strength
                own[1, c, at, :] = mass
                own[2, c, at, :] = conc
            return carry

        lax.fori_loop(0, count, body, 0)

    def exchange(slot, r0, height, c0, w):
        part = (pl.ds(0, 3), pl.ds(c0, w), pl.ds(r0, height))
        return pltpu.make_async_remote_copy(
            src_ref=own.at[part],
            dst_ref=other.at[part],
            send_sem=x_send.at[slot],
            recv_sem=x_recv.at[slot],
            device_id=partner,
            device_id_type=MESH,
        )

    strips = []
    for c, heights in ((0, LEFT), (tiles - 1, RIGHT)):
        for k, height in enumerate(heights):
            strips.append((sum(heights[:k]), height, c))

    def strip(k):
        r0, height, c = strips[k]
        return exchange(k, r0, height, c, 1)

    def send_strip(k):
        r0, height, c = strips[k]
        partial(r0, height // BLOCK, c, 1)
        strip(k).start()

    ends = (
        exchange(len(strips), 0, EDGE, 1, inner),
        exchange(len(strips) + 1, rows - EDGE, EDGE, 1, inner),
    )
    final = exchange(len(strips) + 2, rows - EDGE - FINAL, FINAL, 1, inner)

    def middle(e):
        r = pl.multiple_of(EDGE + e * (PAIR * CHUNK), EDGE)
        return exchange(len(strips) + 3 + e, r, PAIR * CHUNK, 1, inner)

    tail_rows = [EDGE + events * CHUNK + sum(TAIL[:k]) for k in range(len(TAIL))]
    tail = [
        exchange(len(strips) + 3 + events // PAIR + k, r0, height, 1, inner)
        for k, (r0, height) in enumerate(zip(tail_rows, TAIL))
    ]

    def total(r0, count, c0, w):
        for k in range(count):
            r = pl.multiple_of(r0 + k * EDGE, EDGE)
            at = pl.ds(r, EDGE)
            target = pl.ds(pl.multiple_of(r + TOP, EDGE), EDGE)
            for f in range(3):
                for c in range(c0, c0 + w):
                    field[f, c, target, :] = own[f, c, at, :] + other[f, c, at, :]

    weight_load.wait()
    loaded(0)
    load(2)
    partial(0, LEFT[0] // BLOCK, 0, 1)
    pl.semaphore_wait(barrier, before)
    strip(0).start()
    load(3, 4)
    greet(ready, (north, has_north), (west, has_west))
    loaded(1)
    send_strip(1)
    loaded(2)
    for k in range(2, len(LEFT)):
        send_strip(k)

    land_load = pltpu.make_async_copy(land_hbm, land, load_sem.at[15])
    land_load.start()
    field_loads = []
    for k, (f, ref) in enumerate(
        (
            (FU, u_hbm),
            (FV, v_hbm),
            (FA, s1_hbm),
            (FB, s2_hbm),
            (FT, s3_hbm),
            (FX, wx_hbm),
            (FY, wy_hbm),
            (FD, drag_hbm),
        )
    ):
        for c in range(tiles):
            copy = pltpu.make_async_copy(
                ref.at[:, pl.ds(c * LANES, LANES)],
                field.at[f, c, pl.ds(TOP, rows)],
                field_sem.at[k * tiles + c],
            )
            copy.start()
            field_loads.append(copy)

    @pl.when(jnp.logical_not(has_north))
    def _():
        field[:, :, pl.ds(TOP - EDGE, EDGE), :] = jnp.zeros((FIELDS, tiles + 1, EDGE, LANES), jnp.float32)

    @pl.when(jnp.logical_not(has_south))
    def _():
        field[:, :, pl.ds(TOP + rows, EDGE), :] = jnp.zeros((FIELDS, tiles + 1, EDGE, LANES), jnp.float32)

    loaded(3)
    for k in range(len(LEFT), len(strips)):
        send_strip(k)
    loaded(4)
    partial(0, 1, 1, inner)
    ends[0].start()
    partial(rows - BLOCK, 1, 1, inner)
    ends[1].start()

    def send_middle(e, carry):
        partial(BLOCK + e * (PAIR * CHUNK), PAIR * CHUNK // BLOCK, 1, inner)
        middle(e).start()
        return carry

    lax.fori_loop(0, events // PAIR, send_middle, 0)
    reached = BLOCK + events * CHUNK
    partial(reached, (rows - BLOCK - reached) // BLOCK, 1, inner)
    for copy in tail:
        copy.start()
    final.start()

    land_load.wait()

    def wet_body(i, carry):
        r = pl.multiple_of(i * BLOCK, BLOCK)
        for c in range(tiles):
            field[FW, c, pl.ds(pl.multiple_of(r + TOP, EDGE), BLOCK), :] = land[
                pl.ds(r, BLOCK), pl.ds(c * LANES, LANES)
            ].astype(jnp.float32)
        return carry

    lax.fori_loop(0, rows // BLOCK, wet_body, 0)
    for copy in field_loads:
        copy.wait()

    def lon_start(entries, buffers, slot):
        left_out, right_out, left_in, right_in = buffers

        def body(i, carry):
            r = pl.multiple_of(i * CHUNK, 8)
            lane = lax.broadcasted_iota(jnp.int32, (CHUNK, LANES), 1)
            left = right = None
            for k, (f, offset) in enumerate(entries):
                source = pl.ds(pl.multiple_of(r + (TOP + offset), 8), CHUNK)
                x = field[f, 0, source, :]
                y = field[f, tiles - 1, source, :]
                if k == 0:
                    left, right = x, y
                else:
                    shift = EDGE * k
                    left = jnp.where(lane >= shift, pltpu.roll(x, shift, 1), left)
                    right = jnp.where(lane < LANES - shift, pltpu.roll(y, LANES - shift, 1), right)
            left_out[pl.ds(r, CHUNK), :] = left
            right_out[pl.ds(r, CHUNK), :] = right
            return carry

        lax.fori_loop(0, left_out.shape[0] // CHUNK, body, 0)
        copies = tuple(
            pltpu.make_async_remote_copy(
                src_ref=source,
                dst_ref=target,
                send_sem=halo_send.at[slot + k],
                recv_sem=halo_recv.at[slot + k],
                device_id=device,
                device_id_type=MESH,
            )
            for k, (source, target, device) in enumerate(
                ((right_out, left_in, east), (left_out, right_in, west))
            )
        )
        for copy in copies:
            copy.start()
        return copies

    def lon_finish(entries, buffers, copies):
        left_in, right_in = buffers[2:]
        for copy in copies:
            copy.wait()

        def body(i, carry):
            r = pl.multiple_of(i * CHUNK, 8)
            lane = lax.broadcasted_iota(jnp.int32, (CHUNK, LANES), 1)
            x = right_in[pl.ds(r, CHUNK), :]
            y = left_in[pl.ds(r, CHUNK), :]
            for k, (f, offset) in enumerate(entries):
                a = pltpu.roll(x, LANES - EDGE * k, 1) if k else x
                b = pltpu.roll(y, EDGE * k, 1) if k else y
                target = pl.ds(pl.multiple_of(r + (TOP + offset), 8), CHUNK)
                field[f, halo, target, :] = jnp.where(
                    lane < EDGE, a, jnp.where(lane >= LANES - EDGE, b, 0.0)
                )
            return carry

        lax.fori_loop(0, left_in.shape[0] // CHUNK, body, 0)

    def lat_start(first, count, slot):
        def row_copy(source, target, at, device):
            return pltpu.make_async_remote_copy(
                src_ref=field.at[pl.ds(first, count), :, pl.ds(source, EDGE), :],
                dst_ref=field.at[pl.ds(first, count), :, pl.ds(target, EDGE), :],
                send_sem=halo_send.at[at],
                recv_sem=halo_recv.at[at],
                device_id=device,
                device_id_type=MESH,
            )

        to_north = row_copy(TOP, TOP + rows, slot, north)
        to_south = row_copy(TOP + rows - EDGE, TOP - EDGE, slot + 1, south)

        @pl.when(has_north)
        def _():
            to_north.start()

        @pl.when(has_south)
        def _():
            to_south.start()

        return to_north, to_south

    def lat_finish(to_north, to_south):
        @pl.when(has_north)
        def _():
            to_north.wait_send()
            to_south.wait_recv()

        @pl.when(has_south)
        def _():
            to_south.wait_send()
            to_north.wait_recv()

    wide_pack = (pack_left, pack_right, from_left, from_right)
    input_entries = [(f, 0) for f in range(3, FIELDS)]

    @pl.when(after > 0)
    def _():
        pl.semaphore_wait(ready, after)

    @pl.when(has_west)
    def _():
        pl.semaphore_wait(token.at[0], 1)

    @pl.when(has_east)
    def _():
        pl.semaphore_signal(token.at[0], inc=1, device_id=east, device_id_type=MESH)
        pl.semaphore_wait(token.at[1], 1)

    @pl.when(has_west)
    def _():
        pl.semaphore_signal(token.at[1], inc=1, device_id=west, device_id_type=MESH)

    input_copies = lon_start(input_entries, wide_pack, 0)
    lon_finish(input_entries, wide_pack, input_copies)
    input_rows = lat_start(3, FIELDS - 3, 2)

    for k, (r0, height, c) in enumerate(strips):
        strip(k).wait()

        def sum_body(i, carry):
            total(r0 + i * BLOCK, BLOCK // EDGE, c, 1)
            return carry

        lax.fori_loop(0, height // BLOCK, sum_body, 0)
    for copy, r0 in zip(ends, (0, rows - EDGE)):
        copy.wait()
        total(r0, 1, 1, inner)
    short = rows // FOLD
    sum_pack = (sum_left, sum_right, sum_from_left, sum_from_right)
    sum_entries = [(f, g * short) for g in range(FOLD) for f in range(3)]
    sum_copies = lon_start(sum_entries, sum_pack, 4)
    lon_finish(sum_entries, sum_pack, sum_copies)
    sum_rows = lat_start(0, 3, 6)
    lat_finish(*input_rows)
    lat_finish(*sum_rows)

    bottom = TOP + rows - EDGE
    for k in range(2):
        derive(field, bottom + EDGE * k)
    sweep(field, outs, bottom, 2, lambda h: h, None, skip=(1,))

    middle(0).wait()
    total(EDGE, CHUNK // EDGE, 1, inner)
    count = CHUNK // EDGE + 2
    for k in range(count):
        derive(field, TOP - EDGE + EDGE * k)
    sweep(field, outs, TOP - EDGE, count, None, lambda h: EDGE - h, skip=(0,))

    def advance(r, height):
        total(r, height // EDGE, 1, inner)
        for k in range(height // EDGE):
            derive(field, TOP + r + EDGE * k)
        sweep(
            field,
            outs,
            TOP + r - EDGE,
            height // EDGE + 1,
            lambda h: EDGE - h,
            lambda h: EDGE - h,
        )

    def event(e, carry):
        @pl.when(lax.rem(e, PAIR) == 0)
        def _():
            middle(e // PAIR).wait()

        advance(EDGE + e * CHUNK, CHUNK)
        return carry

    lax.fori_loop(1, events, event, 0)
    for copy, r0, height in zip(tail, tail_rows, TAIL):
        copy.wait()
        advance(r0, height)
    final.wait()
    total(rows - EDGE - FINAL, FINAL // EDGE, 1, inner)


def finish(*refs):
    sem = refs[-1]
    results = refs[6:11]
    field = refs[11]
    outs = refs[12:17]
    rows = outs[0].shape[0]
    cone = FINAL + 2 * EDGE
    done = rows - cone

    def write(k, r0, height, slot):
        at = pl.ds(r0, height)
        return pltpu.make_async_copy(outs[k].at[at], results[k].at[at], sem.at[slot])

    early = [write(k, 0, done, k) for k in range(5)]
    for copy in early:
        copy.start()
    start = TOP + done
    for k in range(FINAL // EDGE):
        derive(field, start + EDGE + EDGE * k)
    late = [write(k, done, cone, 5 + k) for k in range(5)]

    def write_stress():
        for copy in late[2:]:
            copy.start()

    sweep(field, outs, start, cone // EDGE, lambda h: EDGE - h, lambda h: h, between=write_stress, unroll=True)
    for copy in late[:2]:
        copy.start()
    for copy in early + late:
        copy.wait()


def shards(
    lat_count,
    lon_count,
    thickness,
    area,
    ridge_weight,
    cat_top,
    land_mask,
    velocity_u,
    velocity_v,
    stress_div,
    stress_ten,
    stress_shear,
    wind_x,
    wind_y,
    water_drag,
):
    cats, rows, cols = thickness.shape
    tiles = cols // LANES
    tall = rows + 2 * TOP
    f32 = jnp.float32
    events = (rows - 2 * EDGE - FINAL - sum(TAIL)) // CHUNK
    slots = len(LEFT) + len(RIGHT) + 3 + events // PAIR + len(TAIL)
    anywhere = pl.BlockSpec(memory_space=pl.ANY)
    vmem = pl.BlockSpec(memory_space=pltpu.VMEM)
    state = (pltpu.VMEM((FIELDS, tiles + 1, tall, LANES), f32),) + tuple(
        pltpu.VMEM((rows, cols), f32) for _ in range(5)
    )
    results = pl.pallas_call(
        functools.partial(kernel, lat_count, lon_count),
        out_shape=state,
        in_specs=[anywhere] * 13,
        out_specs=(vmem,) * 6,
        scratch_shapes=[
            pltpu.SMEM((cats,), f32),
            pltpu.VMEM((3, tiles, rows, LANES), f32),
            pltpu.VMEM((3, tiles, rows, LANES), f32),
            pltpu.VMEM((cats, rows, cols), thickness.dtype),
            pltpu.VMEM((cats, rows, cols), area.dtype),
            pltpu.VMEM((rows, cols), jnp.int32),
            pltpu.VMEM((rows, cols), jnp.int32),
            pltpu.VMEM((rows, LANES), f32),
            pltpu.VMEM((rows, LANES), f32),
            pltpu.VMEM((rows, LANES), f32),
            pltpu.VMEM((rows, LANES), f32),
            pltpu.VMEM((rows // FOLD, LANES), f32),
            pltpu.VMEM((rows // FOLD, LANES), f32),
            pltpu.VMEM((rows // FOLD, LANES), f32),
            pltpu.VMEM((rows // FOLD, LANES), f32),
            pltpu.SemaphoreType.DMA((17,)),
            pltpu.SemaphoreType.DMA((8 * tiles,)),
            pltpu.SemaphoreType.DMA((slots,)),
            pltpu.SemaphoreType.DMA((slots,)),
            pltpu.SemaphoreType.DMA((8,)),
            pltpu.SemaphoreType.DMA((8,)),
            pltpu.SemaphoreType.REGULAR,
            pltpu.SemaphoreType.REGULAR((2,)),
        ],
        compiler_params=pltpu.CompilerParams(
            collective_id=0, has_side_effects=True, vmem_limit_bytes=44 * 2**20
        ),
        name="ice",
    )(
        ridge_weight,
        thickness,
        area,
        cat_top,
        land_mask,
        velocity_u,
        velocity_v,
        stress_div,
        stress_ten,
        stress_shear,
        wind_x,
        wind_y,
        water_drag,
    )
    return pl.pallas_call(
        finish,
        out_shape=tuple(jax.ShapeDtypeStruct((rows, cols), f32) for _ in range(5)) + state,
        in_specs=[vmem] * 6,
        out_specs=(anywhere,) * 5 + (vmem,) * 6,
        input_output_aliases={k: 5 + k for k in range(6)},
        scratch_shapes=[pltpu.SemaphoreType.DMA((10,))],
        compiler_params=pltpu.CompilerParams(vmem_limit_bytes=4 * 2**20),
        name="finish",
    )(*results)[:5]


def solution(mesh):
    body = functools.partial(shards, mesh.shape["lat"], mesh.shape["lon"])
    plane = P("lat", "lon")
    return jax.shard_map(
        body,
        mesh=mesh,
        in_specs=(P("cat", "lat", "lon"), P("cat", "lat", "lon"), P("cat")) + (plane,) * 10,
        out_specs=(plane,) * 5,
        check_vma=False,
    )
```

```python
import functools

import jax
import jax.numpy as jnp
from jax import lax
from jax.experimental import pallas as pl
from jax.experimental.pallas import tpu as pltpu
from jax.sharding import PartitionSpec as P

SUB = 4
LANES = 128
EDGE = 8
BLOCK = 16
CHUNK = 32
TAIL = (16, 16)
FINAL = 16
TOP = 16
LEFT = (16, 48, 192)
RIGHT = (256,)
PAIR = 1
FOLD = 4
MESH = pl.DeviceIdType.MESH

FS, FM, FC, FD, FX, FY, FW, FU, FV, FA, FB, FT = range(12)
FIELDS = 12
THIRD = 1.0 / 3.0


def read(field, f, c, r, shift=0):
    if shift == 0:
        return field[f, c, pl.ds(pl.multiple_of(r, EDGE), EDGE), :]
    near = field.at[f, c, pl.ds(pl.multiple_of(r - EDGE, EDGE), 3 * EDGE)]
    return near[EDGE + shift : 2 * EDGE + shift, :]


def put(ref, value, mask):
    if mask is None:
        ref[...] = value
    else:
        pltpu.store(ref, value, mask=mask)


def along(x, lane):
    tiles = len(x)
    ahead = [pltpu.roll(a, LANES - 1, 1) for a in x]
    behind = [pltpu.roll(a, 1, 1) for a in x]
    return [
        jnp.where(lane == LANES - 1, ahead[(c + 1) % tiles], ahead[c])
        - jnp.where(lane == 0, behind[c - 1], behind[c])
        for c in range(tiles)
    ]


def derive(field, r):
    tiles = field.shape[1]
    at = pl.ds(pl.multiple_of(r, EDGE), EDGE)
    for c in range(tiles):
        wet = field[FW, c, at, :]
        mass = field[FM, c, at, :]
        ratio = wet / (mass + field[FD, c, at, :] + 1.0 - wet)
        force = field[FC, c, at, :] * ratio
        field[FS, c, at, :] = (2.0 * THIRD) * wet * field[FS, c, at, :]
        field[FM, c, at, :] = mass * ratio
        field[FD, c, at, :] = 0.25 * ratio
        field[FX, c, at, :] = force * field[FX, c, at, :]
        field[FY, c, at, :] = force * field[FY, c, at, :]
        field[FW, c, at, :] = THIRD * wet
        first = field[FA, c, at, :]
        second = field[FB, c, at, :]
        field[FA, c, at, :] = first + second
        field[FB, c, at, :] = first - second
        field[FT, c, at, :] = 2.0 * field[FT, c, at, :]


def stress(field, outs, r, mask, lane):
    tiles = field.shape[1]
    at = pl.ds(pl.multiple_of(r, EDGE), EDGE)
    dxu = along([field[FU, c, at, :] for c in range(tiles)], lane)
    dxv = along([field[FV, c, at, :] for c in range(tiles)], lane)
    for c in range(tiles):
        dyu = read(field, FU, c, r, 1) - read(field, FU, c, r, -1)
        dyv = read(field, FV, c, r, 1) - read(field, FV, c, r, -1)
        div = dxu[c] + dyv
        ten = dxu[c] - dyv
        shr = dyu + dxv[c]
        inverse = lax.rsqrt(div * div + 0.25 * (ten * ten + shr * shr) + 0.01)
        power = field[FS, c, at, :]
        keep = field[FW, c, at, :]
        gain = power * inverse
        p = gain * div - power
        q = (0.25 * gain) * ten
        a = keep * field[FA, c, at, :] + (p + q)
        b = keep * field[FB, c, at, :] + (p - q)
        s = keep * field[FT, c, at, :] + (0.5 * gain) * shr
        put(field.at[FA, c, at], a, mask)
        put(field.at[FB, c, at], b, mask)
        put(field.at[FT, c, at], s, mask)
        if outs is not None and c < tiles - 1:
            spot = (pl.ds(pl.multiple_of(r - TOP, EDGE), EDGE), pl.ds(c * LANES, LANES))
            put(outs[2].at[spot], 0.5 * (a + b), mask)
            put(outs[3].at[spot], 0.5 * (a - b), mask)
            put(outs[4].at[spot], 0.5 * s, mask)


def motion(field, outs, r, mask, lane):
    tiles = field.shape[1]
    at = pl.ds(pl.multiple_of(r, EDGE), EDGE)
    dxa = along([field[FA, c, at, :] for c in range(tiles)], lane)
    dxt = along([field[FT, c, at, :] for c in range(tiles)], lane)
    for c in range(tiles):
        fx = dxa[c] + (read(field, FT, c, r, 1) - read(field, FT, c, r, -1))
        fy = dxt[c] + (read(field, FB, c, r, 1) - read(field, FB, c, r, -1))
        u = field[FU, c, at, :]
        v = field[FV, c, at, :]
        inertia = field[FM, c, at, :]
        ratio = field[FD, c, at, :]
        new_u = inertia * (u + 0.5 * v) + ratio * fx + field[FX, c, at, :]
        new_v = inertia * (v - 0.5 * u) + ratio * fy + field[FY, c, at, :]
        put(field.at[FU, c, at], new_u, mask)
        put(field.at[FV, c, at], new_v, mask)
        if outs is not None and c < tiles - 1:
            spot = (pl.ds(pl.multiple_of(r - TOP, EDGE), EDGE), pl.ds(c * LANES, LANES))
            put(outs[0].at[spot], new_u, mask)
            put(outs[1].at[spot], new_v, mask)


def sweep(field, outs, start, count, head, tail, skip=(), between=None, unroll=False):
    lane = lax.broadcasted_iota(jnp.int32, (EDGE, LANES), 1)
    line = lax.broadcasted_iota(jnp.int32, (EDGE, LANES), 0)

    def half(step, h, emit):
        for k in range(count):
            mask = None
            if k == 0 and head is not None:
                mask = line >= head(h)
            if k == count - 1 and tail is not None:
                mask = line < tail(h)
            step(field, outs if emit and k not in skip else None, start + EDGE * k, mask, lane)

    def cycle(t, carry):
        half(stress, 2 * t, False)
        half(motion, 2 * t + 1, False)
        return carry

    if unroll:
        for t in range(SUB - 1):
            cycle(t, 0)
    else:
        lax.fori_loop(0, SUB - 1, cycle, 0)
    half(stress, 2 * SUB - 2, True)
    if between is not None:
        between()
    half(motion, 2 * SUB - 1, True)


def kernel(
    lat_count,
    lon_count,
    weight_hbm,
    thick_hbm,
    area_hbm,
    top_hbm,
    land_hbm,
    u_hbm,
    v_hbm,
    s1_hbm,
    s2_hbm,
    s3_hbm,
    wx_hbm,
    wy_hbm,
    drag_hbm,
    field,
    out_u,
    out_v,
    out_1,
    out_2,
    out_3,
    weight,
    own,
    other,
    thick,
    area,
    top,
    land,
    pack_left,
    pack_right,
    from_left,
    from_right,
    sum_left,
    sum_right,
    sum_from_left,
    sum_from_right,
    load_sem,
    field_sem,
    x_send,
    x_recv,
    halo_send,
    halo_recv,
    ready,
    token,
):
    outs = (out_u, out_v, out_1, out_2, out_3)
    cats, rows, cols = thick.shape
    tiles = cols // LANES
    halo = tiles
    inner = tiles - 2
    last = cols - LANES
    events = (rows - 2 * EDGE - FINAL - sum(TAIL)) // CHUNK
    my_cat = lax.axis_index("cat")
    my_lat = lax.axis_index("lat")
    my_lon = lax.axis_index("lon")
    partner = {"cat": 1 - my_cat}
    west = {"lon": lax.rem(my_lon + lon_count - 1, lon_count)}
    east = {"lon": lax.rem(my_lon + 1, lon_count)}
    north = {"lat": my_lat - 1}
    south = {"lat": my_lat + 1}
    has_north = my_lat > 0
    has_south = my_lat < lat_count - 1


    groups = (
        (0, LEFT[0], 0, LANES),
        (LEFT[0], LEFT[1], 0, LANES),
        (LEFT[0] + LEFT[1], rows - LEFT[0] - LEFT[1], 0, LANES),
        (0, rows, last, LANES),
        (0, rows, LANES, cols - 2 * LANES),
    )
    loads = []
    for k, (r0, height, c0, w) in enumerate(groups):
        spot = (pl.ds(r0, height), pl.ds(c0, w))
        group = (
            pltpu.make_async_copy(top_hbm.at[spot], top.at[spot], load_sem.at[3 * k]),
            pltpu.make_async_copy(
                thick_hbm.at[(slice(None),) + spot], thick.at[(slice(None),) + spot], load_sem.at[3 * k + 1]
            ),
            pltpu.make_async_copy(
                area_hbm.at[(slice(None),) + spot], area.at[(slice(None),) + spot], load_sem.at[3 * k + 2]
            ),
        )
        loads.append(group)

    def load(*which):
        for k in which:
            for copy in loads[k]:
                copy.start()

    def loaded(k):
        for copy in loads[k]:
            copy.wait()

    load(0)
    weight_load = pltpu.make_async_copy(weight_hbm, weight, load_sem.at[16])
    weight_load.start()
    load(1, 2)

    has_west = my_lon > 0
    has_east = my_lon < lon_count - 1
    before = 1 + has_north.astype(jnp.int32) + has_west.astype(jnp.int32)
    after = has_south.astype(jnp.int32) + has_east.astype(jnp.int32)
    barrier = pltpu.get_barrier_semaphore()
    pl.semaphore_signal(barrier, inc=1, device_id=partner, device_id_type=MESH)

    def greet(semaphore, *devices):
        for device, there in devices:

            @pl.when(there)
            def _():
                pl.semaphore_signal(semaphore, inc=1, device_id=device, device_id_type=MESH)

    greet(barrier, (south, has_south), (east, has_east))
    base = my_cat * cats

    def partial(r0, count, c0, w):
        def body(i, carry):
            r = pl.multiple_of(r0 + i * BLOCK, BLOCK)
            at = pl.ds(r, BLOCK)
            for c in range(c0, c0 + w):
                lanes = pl.ds(c * LANES, LANES)
                limit = top[at, lanes] - base
                strength = mass = conc = jnp.zeros((BLOCK, LANES), jnp.float32)
                for n in range(cats):
                    height = thick[n, at, lanes].astype(jnp.float32)
                    cover = jnp.where(limit > n, area[n, at, lanes].astype(jnp.float32), 0.0)
                    volume = cover * height
                    conc = conc + cover
                    mass = mass + volume
                    strength = strength + weight[n] * (volume * height)
                own[0, c, at, :] = strength
                own[1, c, at, :] = mass
                own[2, c, at, :] = conc
            return carry

        lax.fori_loop(0, count, body, 0)

    def exchange(slot, r0, height, c0, w):
        part = (pl.ds(0, 3), pl.ds(c0, w), pl.ds(r0, height))
        return pltpu.make_async_remote_copy(
            src_ref=own.at[part],
            dst_ref=other.at[part],
            send_sem=x_send.at[slot],
            recv_sem=x_recv.at[slot],
            device_id=partner,
            device_id_type=MESH,
        )

    strips = []
    for c, heights in ((0, LEFT), (tiles - 1, RIGHT)):
        for k, height in enumerate(heights):
            strips.append((sum(heights[:k]), height, c))

    def strip(k):
        r0, height, c = strips[k]
        return exchange(k, r0, height, c, 1)

    def send_strip(k):
        r0, height, c = strips[k]
        partial(r0, height // BLOCK, c, 1)
        strip(k).start()

    ends = (
        exchange(len(strips), 0, EDGE, 1, inner),
        exchange(len(strips) + 1, rows - EDGE, EDGE, 1, inner),
    )
    final = exchange(len(strips) + 2, rows - EDGE - FINAL, FINAL, 1, inner)

    def middle(e):
        r = pl.multiple_of(EDGE + e * (PAIR * CHUNK), EDGE)
        return exchange(len(strips) + 3 + e, r, PAIR * CHUNK, 1, inner)

    tail_rows = [EDGE + events * CHUNK + sum(TAIL[:k]) for k in range(len(TAIL))]
    tail = [
        exchange(len(strips) + 3 + events // PAIR + k, r0, height, 1, inner)
        for k, (r0, height) in enumerate(zip(tail_rows, TAIL))
    ]

    def total(r0, count, c0, w):
        for k in range(count):
            r = pl.multiple_of(r0 + k * EDGE, EDGE)
            at = pl.ds(r, EDGE)
            target = pl.ds(pl.multiple_of(r + TOP, EDGE), EDGE)
            for f in range(3):
                for c in range(c0, c0 + w):
                    field[f, c, target, :] = own[f, c, at, :] + other[f, c, at, :]

    weight_load.wait()
    loaded(0)
    partial(0, LEFT[0] // BLOCK, 0, 1)
    pl.semaphore_wait(barrier, before)
    strip(0).start()
    load(3, 4)
    greet(ready, (north, has_north), (west, has_west))
    loaded(1)
    send_strip(1)
    loaded(2)
    for k in range(2, len(LEFT)):
        send_strip(k)

    land_load = pltpu.make_async_copy(land_hbm, land, load_sem.at[15])
    land_load.start()
    field_loads = []
    for k, (f, ref) in enumerate(
        (
            (FU, u_hbm),
            (FV, v_hbm),
            (FA, s1_hbm),
            (FB, s2_hbm),
            (FT, s3_hbm),
            (FX, wx_hbm),
            (FY, wy_hbm),
            (FD, drag_hbm),
        )
    ):
        for c in range(tiles):
            copy = pltpu.make_async_copy(
                ref.at[:, pl.ds(c * LANES, LANES)],
                field.at[f, c, pl.ds(TOP, rows)],
                field_sem.at[k * tiles + c],
            )
            copy.start()
            field_loads.append(copy)

    @pl.when(jnp.logical_not(has_north))
    def _():
        field[:, :, pl.ds(TOP - EDGE, EDGE), :] = jnp.zeros((FIELDS, tiles + 1, EDGE, LANES), jnp.float32)

    @pl.when(jnp.logical_not(has_south))
    def _():
        field[:, :, pl.ds(TOP + rows, EDGE), :] = jnp.zeros((FIELDS, tiles + 1, EDGE, LANES), jnp.float32)

    loaded(3)
    for k in range(len(LEFT), len(strips)):
        send_strip(k)
    loaded(4)
    partial(0, 1, 1, inner)
    ends[0].start()
    partial(rows - BLOCK, 1, 1, inner)
    ends[1].start()

    def send_middle(e, carry):
        partial(BLOCK + e * (PAIR * CHUNK), PAIR * CHUNK // BLOCK, 1, inner)
        middle(e).start()
        return carry

    lax.fori_loop(0, events // PAIR, send_middle, 0)
    reached = BLOCK + events * CHUNK
    partial(reached, (rows - BLOCK - reached) // BLOCK, 1, inner)
    for copy in tail:
        copy.start()
    final.start()

    land_load.wait()

    def wet_body(i, carry):
        r = pl.multiple_of(i * BLOCK, BLOCK)
        for c in range(tiles):
            field[FW, c, pl.ds(pl.multiple_of(r + TOP, EDGE), BLOCK), :] = land[
                pl.ds(r, BLOCK), pl.ds(c * LANES, LANES)
            ].astype(jnp.float32)
        return carry

    lax.fori_loop(0, rows // BLOCK, wet_body, 0)
    for copy in field_loads:
        copy.wait()

    def lon_start(entries, buffers, slot):
        left_out, right_out, left_in, right_in = buffers

        def body(i, carry):
            r = pl.multiple_of(i * CHUNK, 8)
            lane = lax.broadcasted_iota(jnp.int32, (CHUNK, LANES), 1)
            left = right = None
            for k, (f, offset) in enumerate(entries):
                source = pl.ds(pl.multiple_of(r + (TOP + offset), 8), CHUNK)
                x = field[f, 0, source, :]
                y = field[f, tiles - 1, source, :]
                if k == 0:
                    left, right = x, y
                else:
                    shift = EDGE * k
                    left = jnp.where(lane >= shift, pltpu.roll(x, shift, 1), left)
                    right = jnp.where(lane < LANES - shift, pltpu.roll(y, LANES - shift, 1), right)
            left_out[pl.ds(r, CHUNK), :] = left
            right_out[pl.ds(r, CHUNK), :] = right
            return carry

        lax.fori_loop(0, left_out.shape[0] // CHUNK, body, 0)
        copies = tuple(
            pltpu.make_async_remote_copy(
                src_ref=source,
                dst_ref=target,
                send_sem=halo_send.at[slot + k],
                recv_sem=halo_recv.at[slot + k],
                device_id=device,
                device_id_type=MESH,
            )
            for k, (source, target, device) in enumerate(
                ((right_out, left_in, east), (left_out, right_in, west))
            )
        )
        for copy in copies:
            copy.start()
        return copies

    def lon_finish(entries, buffers, copies):
        left_in, right_in = buffers[2:]
        for copy in copies:
            copy.wait()

        def body(i, carry):
            r = pl.multiple_of(i * CHUNK, 8)
            lane = lax.broadcasted_iota(jnp.int32, (CHUNK, LANES), 1)
            x = right_in[pl.ds(r, CHUNK), :]
            y = left_in[pl.ds(r, CHUNK), :]
            for k, (f, offset) in enumerate(entries):
                a = pltpu.roll(x, LANES - EDGE * k, 1) if k else x
                b = pltpu.roll(y, EDGE * k, 1) if k else y
                target = pl.ds(pl.multiple_of(r + (TOP + offset), 8), CHUNK)
                field[f, halo, target, :] = jnp.where(
                    lane < EDGE, a, jnp.where(lane >= LANES - EDGE, b, 0.0)
                )
            return carry

        lax.fori_loop(0, left_in.shape[0] // CHUNK, body, 0)

    def lat_start(first, count, slot):
        def row_copy(source, target, at, device):
            return pltpu.make_async_remote_copy(
                src_ref=field.at[pl.ds(first, count), :, pl.ds(source, EDGE), :],
                dst_ref=field.at[pl.ds(first, count), :, pl.ds(target, EDGE), :],
                send_sem=halo_send.at[at],
                recv_sem=halo_recv.at[at],
                device_id=device,
                device_id_type=MESH,
            )

        to_north = row_copy(TOP, TOP + rows, slot, north)
        to_south = row_copy(TOP + rows - EDGE, TOP - EDGE, slot + 1, south)

        @pl.when(has_north)
        def _():
            to_north.start()

        @pl.when(has_south)
        def _():
            to_south.start()

        return to_north, to_south

    def lat_finish(to_north, to_south):
        @pl.when(has_north)
        def _():
            to_north.wait_send()
            to_south.wait_recv()

        @pl.when(has_south)
        def _():
            to_south.wait_send()
            to_north.wait_recv()

    wide_pack = (pack_left, pack_right, from_left, from_right)
    input_entries = [(f, 0) for f in range(3, FIELDS)]

    @pl.when(after > 0)
    def _():
        pl.semaphore_wait(ready, after)

    @pl.when(has_west)
    def _():
        pl.semaphore_wait(token.at[0], 1)

    @pl.when(has_east)
    def _():
        pl.semaphore_signal(token.at[0], inc=1, device_id=east, device_id_type=MESH)
        pl.semaphore_wait(token.at[1], 1)

    @pl.when(has_west)
    def _():
        pl.semaphore_signal(token.at[1], inc=1, device_id=west, device_id_type=MESH)

    input_copies = lon_start(input_entries, wide_pack, 0)
    lon_finish(input_entries, wide_pack, input_copies)
    input_rows = lat_start(3, FIELDS - 3, 2)

    for k, (r0, height, c) in enumerate(strips):
        strip(k).wait()

        def sum_body(i, carry):
            total(r0 + i * BLOCK, BLOCK // EDGE, c, 1)
            return carry

        lax.fori_loop(0, height // BLOCK, sum_body, 0)
    for copy, r0 in zip(ends, (0, rows - EDGE)):
        copy.wait()
        total(r0, 1, 1, inner)
    short = rows // FOLD
    sum_pack = (sum_left, sum_right, sum_from_left, sum_from_right)
    sum_entries = [(f, g * short) for g in range(FOLD) for f in range(3)]
    sum_copies = lon_start(sum_entries, sum_pack, 4)
    lon_finish(sum_entries, sum_pack, sum_copies)
    sum_rows = lat_start(0, 3, 6)
    lat_finish(*input_rows)
    lat_finish(*sum_rows)

    bottom = TOP + rows - EDGE
    for k in range(2):
        derive(field, bottom + EDGE * k)
    sweep(field, outs, bottom, 2, lambda h: h, None, skip=(1,))

    middle(0).wait()
    total(EDGE, CHUNK // EDGE, 1, inner)
    count = CHUNK // EDGE + 2
    for k in range(count):
        derive(field, TOP - EDGE + EDGE * k)
    sweep(field, outs, TOP - EDGE, count, None, lambda h: EDGE - h, skip=(0,))

    def advance(r, height):
        total(r, height // EDGE, 1, inner)
        for k in range(height // EDGE):
            derive(field, TOP + r + EDGE * k)
        sweep(
            field,
            outs,
            TOP + r - EDGE,
            height // EDGE + 1,
            lambda h: EDGE - h,
            lambda h: EDGE - h,
        )

    def event(e, carry):
        @pl.when(lax.rem(e, PAIR) == 0)
        def _():
            middle(e // PAIR).wait()

        advance(EDGE + e * CHUNK, CHUNK)
        return carry

    lax.fori_loop(1, events, event, 0)
    for copy, r0, height in zip(tail, tail_rows, TAIL):
        copy.wait()
        advance(r0, height)
    final.wait()
    total(rows - EDGE - FINAL, FINAL // EDGE, 1, inner)


def finish(*refs):
    sem = refs[-1]
    results = refs[6:11]
    field = refs[11]
    outs = refs[12:17]
    rows = outs[0].shape[0]
    cone = FINAL + 2 * EDGE
    done = rows - cone

    def write(k, r0, height, slot):
        at = pl.ds(r0, height)
        return pltpu.make_async_copy(outs[k].at[at], results[k].at[at], sem.at[slot])

    early = [write(k, 0, done, k) for k in range(5)]
    for copy in early:
        copy.start()
    start = TOP + done
    for k in range(FINAL // EDGE):
        derive(field, start + EDGE + EDGE * k)
    late = [write(k, done, cone, 5 + k) for k in range(5)]

    def write_stress():
        for copy in late[2:]:
            copy.start()

    sweep(field, outs, start, cone // EDGE, lambda h: EDGE - h, lambda h: h, between=write_stress, unroll=True)
    for copy in late[:2]:
        copy.start()
    for copy in early + late:
        copy.wait()


def shards(
    lat_count,
    lon_count,
    thickness,
    area,
    ridge_weight,
    cat_top,
    land_mask,
    velocity_u,
    velocity_v,
    stress_div,
    stress_ten,
    stress_shear,
    wind_x,
    wind_y,
    water_drag,
):
    cats, rows, cols = thickness.shape
    tiles = cols // LANES
    tall = rows + 2 * TOP
    f32 = jnp.float32
    events = (rows - 2 * EDGE - FINAL - sum(TAIL)) // CHUNK
    slots = len(LEFT) + len(RIGHT) + 3 + events // PAIR + len(TAIL)
    anywhere = pl.BlockSpec(memory_space=pl.ANY)
    vmem = pl.BlockSpec(memory_space=pltpu.VMEM)
    state = (pltpu.VMEM((FIELDS, tiles + 1, tall, LANES), f32),) + tuple(
        pltpu.VMEM((rows, cols), f32) for _ in range(5)
    )
    results = pl.pallas_call(
        functools.partial(kernel, lat_count, lon_count),
        out_shape=state,
        in_specs=[anywhere] * 13,
        out_specs=(vmem,) * 6,
        scratch_shapes=[
            pltpu.SMEM((cats,), f32),
            pltpu.VMEM((3, tiles, rows, LANES), f32),
            pltpu.VMEM((3, tiles, rows, LANES), f32),
            pltpu.VMEM((cats, rows, cols), thickness.dtype),
            pltpu.VMEM((cats, rows, cols), area.dtype),
            pltpu.VMEM((rows, cols), jnp.int32),
            pltpu.VMEM((rows, cols), jnp.int32),
            pltpu.VMEM((rows, LANES), f32),
            pltpu.VMEM((rows, LANES), f32),
            pltpu.VMEM((rows, LANES), f32),
            pltpu.VMEM((rows, LANES), f32),
            pltpu.VMEM((rows // FOLD, LANES), f32),
            pltpu.VMEM((rows // FOLD, LANES), f32),
            pltpu.VMEM((rows // FOLD, LANES), f32),
            pltpu.VMEM((rows // FOLD, LANES), f32),
            pltpu.SemaphoreType.DMA((17,)),
            pltpu.SemaphoreType.DMA((8 * tiles,)),
            pltpu.SemaphoreType.DMA((slots,)),
            pltpu.SemaphoreType.DMA((slots,)),
            pltpu.SemaphoreType.DMA((8,)),
            pltpu.SemaphoreType.DMA((8,)),
            pltpu.SemaphoreType.REGULAR,
            pltpu.SemaphoreType.REGULAR((2,)),
        ],
        compiler_params=pltpu.CompilerParams(
            collective_id=0, has_side_effects=True, vmem_limit_bytes=44 * 2**20
        ),
        name="ice",
    )(
        ridge_weight,
        thickness,
        area,
        cat_top,
        land_mask,
        velocity_u,
        velocity_v,
        stress_div,
        stress_ten,
        stress_shear,
        wind_x,
        wind_y,
        water_drag,
    )
    return pl.pallas_call(
        finish,
        out_shape=tuple(jax.ShapeDtypeStruct((rows, cols), f32) for _ in range(5)) + state,
        in_specs=[vmem] * 6,
        out_specs=(anywhere,) * 5 + (vmem,) * 6,
        input_output_aliases={k: 5 + k for k in range(6)},
        scratch_shapes=[pltpu.SemaphoreType.DMA((10,))],
        compiler_params=pltpu.CompilerParams(vmem_limit_bytes=4 * 2**20),
        name="finish",
    )(*results)[:5]


def solution(mesh):
    body = functools.partial(shards, mesh.shape["lat"], mesh.shape["lon"])
    plane = P("lat", "lon")
    return jax.shard_map(
        body,
        mesh=mesh,
        in_specs=(P("cat", "lat", "lon"), P("cat", "lat", "lon"), P("cat")) + (plane,) * 10,
        out_specs=(plane,) * 5,
        check_vma=False,
    )
```
